256 devices in a mesh: row: 16 (over y, z_lo, core), col: 16 (over x, z_hi).
Axes of the slice: x: 4, y: 4, z: 8 (z_hi: 4, z_lo: 2; z = z_hi * 2 + z_lo), core: 2. Of those that a mesh axis runs over, the one named last changes fastest.
Arguments:
- start_field: float32 [1, 2, 4096, 8192], P(None, None, 'col', 'row'), may hold values from -6 to 6
- section_field: float32 [1, 2, 4096, 8192], P(None, None, 'col', 'row'), may hold values from -26 to 26
- start_term: float32 [1, 2, 4096, 8192], P(None, None, 'col', 'row'), may hold values from -6 to 6
- first_term: float32 [1, 2, 4096, 8192], P(None, None, 'col', 'row'), may hold values from -6 to 6
- second_term: float32 [1, 2, 4096, 8192], P(None, None, 'col', 'row'), may hold values from -6 to 6
Outputs:
- next_field: float32 [1, 2, 4096, 8192], P(None, None, 'col', 'row')
The draws below stay inside these ranges and needn't reach their ends.
All inputs are finite; a program needn't handle non-finite values.
Results may differ from the reference program's by a relative error of at most 0.0001.
Values sent between devices are 32-bit elements; how exact they have to be, the bound alone decides.
A program may use at most 128 MiB of HBM per device.

```python
import math
import jax
import jax.numpy as jnp
from jax import lax

N = 8192
MEMBERS = 1
NK = 4096


def draw_section_field(key, part):
    wave_x = lax.broadcasted_iota(jnp.int32, (NK, N), 0)
    index_y = lax.broadcasted_iota(jnp.int32, (NK, N), 1)
    wave_y = jnp.where(index_y < N // 2, index_y, index_y - N)
    envelope = 3.0 * jnp.sqrt((wave_x * wave_x + wave_y * wave_y).astype(jnp.float32)) / N
    noise = jnp.clip(jax.random.normal(key, (MEMBERS, 2, NK, N), jnp.float32), -6.0, 6.0)
    return 2.0 * envelope * noise


def steps_of(key, dims, split, smallest, largest):
    factor_of, own = 1.0, jax.random.fold_in(key, 6)
    for dim, blocks in split:
        steps = jnp.exp(jax.random.uniform(jax.random.fold_in(own, dim), (blocks,), jnp.float32, smallest / len(split), largest / len(split)))
        factor_of = factor_of * jnp.repeat(steps, dims[dim] // blocks).reshape([-1 if axis == dim else 1 for axis in range(len(dims))])
    return factor_of


def gaussian(key, extent, deviation, limit, cuts=(), dtype=jnp.bfloat16):
    drawn = deviation * jax.random.normal(key, extent, jnp.float32)
    if cuts:
        drawn = drawn * steps_of(key, extent, cuts, -0.22, 0.18)
    return jnp.clip(drawn, -limit, limit).astype(dtype)


def setup_inputs(seed: int = 0) -> dict:
    seeds = jax.random.split(jax.random.key(seed), 6)
    start_field = gaussian(seeds[0], (MEMBERS, 2, NK, N), 1.0, 6.0, ((2, 16), (3, 16)), jnp.float32)
    section_field = draw_section_field(jax.random.fold_in(seeds[5], 71), 0)
    start_term = gaussian(seeds[2], (MEMBERS, 2, NK, N), 1.0, 6.0, ((2, 16), (3, 16)), jnp.float32)
    first_term = gaussian(seeds[3], (MEMBERS, 2, NK, N), 1.0, 6.0, ((2, 16), (3, 16)), jnp.float32)
    second_term = gaussian(seeds[4], (MEMBERS, 2, NK, N), 1.0, 6.0, ((2, 16), (3, 16)), jnp.float32)
    return dict(start_field=start_field, section_field=section_field, start_term=start_term, first_term=first_term, second_term=second_term)


viscous_rate = 1.5
wave_scale = 3.0
series_terms = 12


def section_weights(wave_x, wave_y, length):
    square = wave_x * wave_x + wave_y * wave_y
    kappa_x = wave_scale * wave_x.astype(jnp.float32) / length
    kappa_y = wave_scale * wave_y.astype(jnp.float32) / length
    kappa_sq = kappa_x * kappa_x + kappa_y * kappa_y
    zvalue = -viscous_rate * kappa_sq
    damping = jnp.exp(zvalue)
    near_zero = 27 * square < 2 * length * length

    def series(degree):
        running = jnp.full_like(zvalue, 1.0 / math.factorial(series_terms - 1 + degree))
        for term_index in range(series_terms - 2, -1, -1):
            running = running * zvalue + 1.0 / math.factorial(term_index + degree)
        return running

    clamped = jnp.where(near_zero, -1.0, zvalue)
    exp_clamped = jnp.exp(clamped)
    closed_one = (exp_clamped - 1.0) / clamped
    closed_two = (exp_clamped - 1.0 - clamped) / (clamped * clamped)
    closed_three = (exp_clamped - 1.0 - clamped - 0.5 * clamped * clamped) / (clamped * clamped * clamped)
    phi_one = jnp.where(near_zero, series(1), closed_one)
    phi_two = jnp.where(near_zero, series(2), closed_two)
    phi_three = jnp.where(near_zero, series(3), closed_three)
    weight_a = phi_one - 3.0 * phi_two + 4.0 * phi_three
    weight_b = phi_two - 2.0 * phi_three
    weight_c = 4.0 * phi_three - phi_two
    keep_mask = ((3 * jnp.abs(wave_x) < length) & (3 * jnp.abs(wave_y) < length)).astype(jnp.float32)
    inverse_sq = (length * length) / (9.0 * jnp.maximum(square, 1).astype(jnp.float32))
    return damping, weight_a, weight_b, weight_c, kappa_x, kappa_y, keep_mask, inverse_sq


def to_grid(real_part, imag_part):
    length = real_part.shape[1]
    complex_spec = lax.complex(real_part, imag_part)
    along_y = jnp.fft.ifft(complex_spec, axis=1)
    return jnp.fft.irfft(along_y, n=length, axis=0) * length


def to_spectrum(real_grid):
    length = real_grid.shape[0]
    along_x = jnp.fft.rfft(real_grid, axis=0)[: length // 2]
    spectrum = jnp.fft.fft(along_x, axis=1) / length
    return jnp.real(spectrum), jnp.imag(spectrum)


def reference(start_field, section_field, start_term, first_term, second_term):
    length = start_field.shape[3]
    wave_x = lax.broadcasted_iota(jnp.int32, (length // 2, length), 0)
    index_y = lax.broadcasted_iota(jnp.int32, (length // 2, length), 1)
    wave_y = jnp.where(index_y < length // 2, index_y, index_y - length)
    damping, weight_a, weight_b, weight_c, kappa_x, kappa_y, keep_mask, inverse_sq = section_weights(wave_x, wave_y, length)
    section_terms = []
    for member in range(section_field.shape[0]):
        real_part = section_field[member, 0] * keep_mask
        imag_part = section_field[member, 1] * keep_mask
        psi_real = real_part * inverse_sq
        psi_imag = imag_part * inverse_sq
        vel_u = to_grid(-kappa_y * psi_imag, kappa_y * psi_real)
        grad_x = to_grid(-kappa_x * imag_part, kappa_x * real_part)
        jacobian = vel_u * grad_x
        vel_v = to_grid(kappa_x * psi_imag, -kappa_x * psi_real)
        grad_y = to_grid(-kappa_y * imag_part, kappa_y * real_part)
        jacobian = jacobian + vel_v * grad_y
        jac_real, jac_imag = to_spectrum(jacobian)
        section_terms.append(jnp.stack([-keep_mask * jac_real, -keep_mask * jac_imag]))
    section_term = jnp.stack(section_terms)
    return damping * start_field + weight_a * start_term + 2.0 * weight_b * (first_term + second_term) + weight_c * section_term
```

```python
import math

import jax
import jax.numpy as jnp
from jax import lax
from jax.experimental import pallas as pl
from jax.experimental.pallas import tpu as pltpu
from jax.sharding import PartitionSpec as P

RADIX = 128


viscous_rate = 1.5
wave_scale = 3.0
series_terms = 12


def section_weights(wave_x, wave_y, length):
    square = wave_x * wave_x + wave_y * wave_y
    kappa_x = wave_scale * wave_x.astype(jnp.float32) / length
    kappa_y = wave_scale * wave_y.astype(jnp.float32) / length
    kappa_sq = kappa_x * kappa_x + kappa_y * kappa_y
    zvalue = -viscous_rate * kappa_sq
    damping = jnp.exp(zvalue)
    near_zero = 27 * square < 2 * length * length

    def series(degree):
        running = jnp.full_like(zvalue, 1.0 / math.factorial(series_terms - 1 + degree))
        for term_index in range(series_terms - 2, -1, -1):
            running = running * zvalue + 1.0 / math.factorial(term_index + degree)
        return running

    clamped = jnp.where(near_zero, -1.0, zvalue)
    exp_clamped = jnp.exp(clamped)
    closed_one = (exp_clamped - 1.0) / clamped
    closed_two = (exp_clamped - 1.0 - clamped) / (clamped * clamped)
    closed_three = (exp_clamped - 1.0 - clamped - 0.5 * clamped * clamped) / (
        clamped * clamped * clamped
    )
    phi_one = jnp.where(near_zero, series(1), closed_one)
    phi_two = jnp.where(near_zero, series(2), closed_two)
    phi_three = jnp.where(near_zero, series(3), closed_three)
    weight_a = phi_one - 3.0 * phi_two + 4.0 * phi_three
    weight_b = phi_two - 2.0 * phi_three
    weight_c = 4.0 * phi_three - phi_two
    keep_mask = ((3 * jnp.abs(wave_x) < length) & (3 * jnp.abs(wave_y) < length)).astype(
        jnp.float32
    )
    inverse_sq = length * length / (9.0 * jnp.maximum(square, 1).astype(jnp.float32))
    return (damping, weight_a, weight_b, weight_c, kappa_x, kappa_y, keep_mask, inverse_sq)


def section_table(count_in, count_out, period, direction):
    row_ids = lax.broadcasted_iota(jnp.int32, (count_in, count_out), 0)
    col_ids = lax.broadcasted_iota(jnp.int32, (count_in, count_out), 1)
    angles = direction * 2.0 * math.pi / period * (row_ids * col_ids % period).astype(jnp.float32)
    cosine = jnp.cos(angles)
    sine_part = jnp.sin(angles)
    return jnp.stack(
        [jnp.stack([cosine, sine_part], axis=1), jnp.stack([-sine_part, cosine], axis=1)], axis=0
    )


def twiddle(count_c, count_b, period, direction):
    row_ids = lax.broadcasted_iota(jnp.int32, (count_c, count_b), 0)
    col_ids = lax.broadcasted_iota(jnp.int32, (count_c, count_b), 1)
    angles = direction * 2.0 * math.pi / period * (row_ids * col_ids % period).astype(jnp.float32)
    return (jnp.cos(angles), jnp.sin(angles))


def rotate(values, cosine, sine_part):
    return jnp.stack(
        [values[0] * cosine - values[1] * sine_part, values[0] * sine_part + values[1] * cosine]
    )


def product(equation, left, right):
    return jnp.einsum(equation, left, right, precision=lax.Precision.HIGH)


def lines_inverse(pieces):
    parts, count_k, length = pieces.shape
    count_b = RADIX
    count_a = length // count_b
    shaped = pieces.reshape((parts, count_k, count_a, count_b))
    first = product("pkab,pasc->skcb", shaped, section_table(count_a, count_a, count_a, 1.0))
    first = rotate(first, *twiddle(count_a, count_b, length, 1.0))
    second = product("pkcb,pbsd->skcd", first, section_table(count_b, count_b, count_b, 1.0))
    return second.reshape((parts, count_k, length))


def lines_forward(pieces):
    parts, count_k, length = pieces.shape
    count_d = RADIX
    count_c = length // count_d
    shaped = pieces.reshape((parts, count_k, count_c, count_d))
    first = product("pkcd,pdsf->skcf", shaped, section_table(count_d, count_d, count_d, -1.0))
    first = rotate(first, *twiddle(count_c, count_d, length, -1.0))
    second = product("pkcf,pcse->skef", first, section_table(count_c, count_c, count_c, -1.0))
    return second.reshape((parts, count_k, length))


def turned_table(count_c, count_b, period, direction):
    c_ids = lax.broadcasted_iota(jnp.int32, (count_c, count_b, count_b), 0)
    b_ids = lax.broadcasted_iota(jnp.int32, (count_c, count_b, count_b), 1)
    d_ids = lax.broadcasted_iota(jnp.int32, (count_c, count_b, count_b), 2)
    steps = b_ids * (c_ids + count_c * d_ids) % period
    angles = direction * 2.0 * math.pi / period * steps.astype(jnp.float32)
    return jnp.cos(angles), jnp.sin(angles)


def columns_inverse(pieces, table):
    parts, half_count, count_y = pieces.shape
    count_a = half_count // RADIX
    count_c = 2 * count_a
    shaped = pieces.reshape((parts, count_a, RADIX, count_y))
    first = product("paby,pasc->csby", shaped, section_table(count_a, count_c, count_c, 1.0))
    return product("csby,csbd->cdy", first, table)


def columns_forward(grid, table):
    count_c, count_d, count_y = grid.shape
    half_count = count_c // 2
    first = product("cdy,cpfd->cpfy", grid, table)
    second = product(
        "cpfy,pcse->sefy", first, section_table(count_c, half_count, count_c, -1.0)
    )
    return second.reshape((2, half_count * count_d, count_y))


def swap_kernel(source, target, send_sem, recv_sem, own_sem):
    row, col = lax.axis_index("row"), lax.axis_index("col")
    rows, cols = lax.axis_size("row"), lax.axis_size("col")
    own = col * rows + row
    keep = pltpu.make_async_copy(source.at[own], target.at[own], own_sem)
    keep.start()

    def send(step, carry):
        peer_row = lax.rem(row + step % rows, rows)
        peer_col = lax.rem(col + step // rows, cols)
        pltpu.make_async_remote_copy(
            source.at[peer_col * rows + peer_row],
            target.at[own],
            send_sem,
            recv_sem,
            device_id={"row": peer_row, "col": peer_col},
            device_id_type=pl.DeviceIdType.MESH,
        ).start()
        return carry

    lax.fori_loop(1, rows * cols, send, 0)
    keep.wait()
    others = target.at[pl.ds(0, rows * cols - 1)]
    pltpu.make_async_copy(others, others, recv_sem).wait()
    pltpu.make_async_copy(others, others, send_sem).wait()


def swap(blocks):
    return pl.pallas_call(
        swap_kernel,
        out_shape=jax.ShapeDtypeStruct(blocks.shape, blocks.dtype),
        in_specs=[pl.BlockSpec(memory_space=pltpu.VMEM)],
        out_specs=pl.BlockSpec(memory_space=pltpu.VMEM),
        scratch_shapes=[pltpu.SemaphoreType.DMA] * 3,
        compiler_params=pltpu.CompilerParams(has_side_effects=True),
    )(blocks)


def to_columns(lines):
    parts, count_k, length = lines.shape
    devices = lax.axis_size("col") * lax.axis_size("row")
    width = length // devices
    blocks = lines.reshape(parts, count_k, devices, width).transpose(2, 0, 1, 3)
    blocks = swap(blocks.reshape(devices, -1, 128))
    blocks = blocks.reshape(devices, parts, count_k, width).transpose(1, 0, 2, 3)
    return blocks.reshape(parts, devices * count_k, width)


def to_lines(columns):
    parts, half_count, width = columns.shape
    devices = lax.axis_size("col") * lax.axis_size("row")
    count_k = half_count // devices
    blocks = columns.reshape(parts, devices, count_k, width).transpose(1, 0, 2, 3)
    blocks = swap(blocks.reshape(devices, -1, 128))
    blocks = blocks.reshape(devices, parts, count_k, width).transpose(1, 2, 0, 3)
    return blocks.reshape(parts, count_k, devices * width)


def positions(shape, start_x, start_y, length):
    wave_x = start_x + lax.broadcasted_iota(jnp.int32, shape, 0)
    index_y = start_y + lax.broadcasted_iota(jnp.int32, shape, 1)
    wave_y = jnp.where(index_y < length // 2, index_y, index_y - length)
    return wave_x, wave_y


def nonlinear(section_field, length):
    block_x = section_field.shape[1]
    lines = lax.all_to_all(section_field, "row", split_axis=1, concat_axis=2, tiled=True)
    count_k = lines.shape[1]
    start_x = lax.axis_index("col") * block_x + lax.axis_index("row") * count_k
    wave_x, wave_y = positions((count_k, length), start_x, 0, length)
    square = wave_x * wave_x + wave_y * wave_y
    kappa_x = wave_scale * wave_x.astype(jnp.float32) / length
    kappa_y = wave_scale * wave_y.astype(jnp.float32) / length
    keep = (3 * jnp.abs(wave_x) < length) & (3 * jnp.abs(wave_y) < length)
    doubled = jnp.where(wave_x == 0, 1.0, 2.0) * (1.0 / length)
    inverse_sq = length * length / (9.0 * jnp.maximum(square, 1).astype(jnp.float32))
    factor = jnp.where(keep, inverse_sq * doubled, 0.0)
    scale_u = kappa_y * factor
    scale_v = kappa_x * factor
    spec_u = jnp.stack([-scale_u * lines[1], scale_u * lines[0]])
    spec_v = jnp.stack([scale_v * lines[1], -scale_v * lines[0]])
    count_c = length // RADIX
    cosine, sine_part = turned_table(count_c, RADIX, length, 1.0)
    table = jnp.stack([cosine, -sine_part], axis=1)
    vel_u = columns_inverse(to_columns(lines_inverse(spec_u)), table)
    vel_v = columns_inverse(to_columns(lines_inverse(spec_v)), table)
    cross = lines_forward(to_lines(columns_forward(vel_u * vel_v, table)))
    square_gap = lines_forward(
        to_lines(columns_forward((vel_v - vel_u) * (vel_v + vel_u), table))
    )
    scale = jnp.where(keep, 1.0 / length, 0.0)
    weight_cross = (kappa_x * kappa_x - kappa_y * kappa_y) * scale
    weight_gap = kappa_x * kappa_y * scale
    term = weight_cross * cross + weight_gap * square_gap
    return lax.all_to_all(term, "row", split_axis=2, concat_axis=1, tiled=True)


def per_device(start_field, section_field, start_term, first_term, second_term):
    members = start_field.shape[0]
    block_x = start_field.shape[2]
    block_y = start_field.shape[3]
    length = block_y * lax.axis_size("row")
    wave_x, wave_y = positions(
        (block_x, block_y),
        lax.axis_index("col") * block_x,
        lax.axis_index("row") * block_y,
        length,
    )
    damping, weight_a, weight_b, weight_c = section_weights(wave_x, wave_y, length)[:4]
    linear = (
        damping * start_field
        + weight_a * start_term
        + 2.0 * weight_b * (first_term + second_term)
    )
    linear, weight_c = lax.optimization_barrier((linear, weight_c))
    section_term = jnp.stack([nonlinear(section_field[m], length) for m in range(members)])
    return linear + weight_c * section_term


def solution(mesh):
    return jax.shard_map(
        per_device,
        mesh=mesh,
        in_specs=(
            P(None, None, "col", "row"),
            P(None, None, "col", "row"),
            P(None, None, "col", "row"),
            P(None, None, "col", "row"),
            P(None, None, "col", "row"),
        ),
        out_specs=P(None, None, "col", "row"),
        check_vma=False,
    )
```

```python
import functools
import math

import jax
import jax.numpy as jnp
import ml_dtypes
import numpy as np
from jax import lax
from jax.experimental import pallas as pl
from jax.experimental.pallas import tpu as pltpu
from jax.sharding import PartitionSpec as P

LENGTH = 8192
ROWS = 16
COLS = 16
DEVICES = ROWS * COLS
BLOCK_X = 256
BLOCK_Y = 512
LINES = 11
KEPT = 12
PAIRS = 33

viscous_rate = 1.5
wave_scale = 3.0
series_terms = 12

HIGH = jnp.bfloat16
FULL = jnp.float32


def section_weights(wave_x, wave_y):
    square = wave_x * wave_x + wave_y * wave_y
    kappa_x = wave_scale * wave_x.astype(FULL) / LENGTH
    kappa_y = wave_scale * wave_y.astype(FULL) / LENGTH
    kappa_sq = kappa_x * kappa_x + kappa_y * kappa_y
    zvalue = -viscous_rate * kappa_sq
    damping = jnp.exp(zvalue)
    near_zero = 27 * square < 2 * LENGTH * LENGTH

    def series(degree):
        running = jnp.full_like(zvalue, 1.0 / math.factorial(series_terms - 1 + degree))
        for term_index in range(series_terms - 2, -1, -1):
            running = running * zvalue + 1.0 / math.factorial(term_index + degree)
        return running

    clamped = jnp.where(near_zero, -1.0, zvalue)
    exp_clamped = jnp.exp(clamped)
    closed_one = (exp_clamped - 1.0) / clamped
    closed_two = (exp_clamped - 1.0 - clamped) / (clamped * clamped)
    closed_three = (exp_clamped - 1.0 - clamped - 0.5 * clamped * clamped) / (
        clamped * clamped * clamped
    )
    phi_one = jnp.where(near_zero, series(1), closed_one)
    phi_two = jnp.where(near_zero, series(2), closed_two)
    phi_three = jnp.where(near_zero, series(3), closed_three)
    weight_a = phi_one - 3.0 * phi_two + 4.0 * phi_three
    weight_b = phi_two - 2.0 * phi_three
    weight_c = 4.0 * phi_three - phi_two
    return damping, weight_a, weight_b, weight_c


def halves(table):
    table = np.asarray(table, np.float32)
    high = table.astype(ml_dtypes.bfloat16)
    low = (table - high.astype(np.float32)).astype(ml_dtypes.bfloat16)
    return np.stack([high, low])


@functools.lru_cache(None)
def tables():
    row = np.arange(KEPT * 8)
    kept_row = row // 8
    source_row = np.where(kept_row < KEPT // 2, kept_row, kept_row + ROWS - KEPT)
    part = row % 8 // 4
    index_a = 4 * source_row + row % 4
    index_c = np.arange(64)
    angle = 2 * np.pi / 64 * (index_c[:, None] * index_a[None, :] % 64)
    cosine, sine = np.cos(angle), np.sin(angle)
    real_rows = np.where(part == 0, -sine, -cosine)
    imag_rows = np.where(part == 0, cosine, -sine)
    first = np.concatenate([real_rows, imag_rows])
    real_out = np.where(part == 0, cosine, -sine)
    imag_out = np.where(part == 0, sine, cosine)
    last = np.concatenate([real_out, imag_out]).T
    index_b = np.arange(128)
    turn = 2 * np.pi / LENGTH * (index_c[:, None] * index_b[None, :])
    turns = np.stack([np.cos(turn), np.sin(turn)]).astype(np.float32)
    angle = 2 * np.pi / 128 * (index_b[:, None] * index_b[None, :] % 128)
    cosine, sine = np.cos(angle), np.sin(angle)
    second = np.zeros((2, 2, 128, 4, 2, 2, 32))
    for field in range(2):
        second[0, field, :, :, 0, field] = cosine.reshape(128, 4, 32)
        second[0, field, :, :, 1, field] = sine.reshape(128, 4, 32)
        second[1, field, :, :, 0, field] = -sine.reshape(128, 4, 32)
        second[1, field, :, :, 1, field] = cosine.reshape(128, 4, 32)
    second = second.reshape(512, 512)
    spin = 2 * np.pi / LENGTH * np.broadcast_to(index_b[None, :], (128, 128))
    base = np.stack(
        [cosine, -sine, np.cos(spin), -np.sin(spin), np.cos(spin.T), -np.sin(spin.T)]
    ).astype(np.float32)
    return halves(first), halves(second), halves(second.T), halves(last), turns, base


def split(values):
    high = values.astype(HIGH)
    return high, (values - high.astype(FULL)).astype(HIGH)


def times(left_high, left_low, right_high, right_low):
    dot = functools.partial(jnp.dot, preferred_element_type=FULL)
    return (
        dot(left_high, right_low) + dot(left_low, right_high)
    ) + dot(left_high, right_high)


def turned(values, upper):
    moved = pltpu.roll(values, 64, 1)
    return jnp.where(upper, moved, -moved)


def cosine_of(step, period):
    return math.cos(2 * math.pi * (step % period) / period)


def sine_of(step, period):
    return math.sin(2 * math.pi * (step % period) / period)


def scaled(factor, value):
    if abs(factor) < 1e-12:
        return None
    if abs(factor - 1) < 1e-12:
        return value
    if abs(factor + 1) < 1e-12:
        return -value
    return factor * value


def total(values):
    values = [value for value in values if value is not None]
    if not values:
        return None
    return functools.reduce(lambda a, b: a + b, values)


def plus(a, b):
    return b if a is None else a if b is None else a + b


def minus(a, b):
    return a if b is None else -b if a is None else a - b


def spread_lines(lines, upper):
    turns = [turned(line, upper) for line in lines]
    out = [None] * 32
    for step in range(9):
        sums = []
        for parity in range(2):
            picked = range(parity, LINES, 2)
            sums.append(total(scaled(cosine_of(l * step, 32), lines[l]) for l in picked))
            sums.append(total(scaled(sine_of(l * step, 32), turns[l]) for l in picked))
        cos_even, sin_even, cos_odd, sin_odd = sums
        cos_sum, cos_gap = plus(cos_even, cos_odd), minus(cos_even, cos_odd)
        sin_sum, sin_gap = plus(sin_even, sin_odd), minus(sin_even, sin_odd)
        out[step] = plus(cos_sum, sin_sum)
        out[(16 + step) % 32] = plus(cos_gap, sin_gap)
        if step:
            out[32 - step] = minus(cos_sum, sin_sum)
            out[16 - step] = minus(cos_gap, sin_gap)
    return out


def gather_lines(points, upper):
    out = [None] * LINES
    for parity in range(2):
        sign = 1 - 2 * parity
        folded = [
            points[step] + points[step + 16] if sign > 0 else points[step] - points[step + 16]
            for step in range(16)
        ]
        even, odd = [folded[0]], [None]
        for step in range(1, 8):
            mirror = folded[16 - step]
            even.append(folded[step] + mirror if sign > 0 else folded[step] - mirror)
            odd.append(
                turned(folded[step] - mirror if sign > 0 else folded[step] + mirror, upper)
            )
        even.append(folded[8])
        odd.append(turned(folded[8], upper))
        for l in range(parity, LINES, 2):
            terms = [scaled(cosine_of(l * step, 32), even[step]) for step in range(9)]
            terms += [scaled(-sine_of(l * step, 32), odd[step]) for step in range(1, 9)]
            out[l] = total(terms)
    return out


def section_kernel(
    start_field,
    section_field,
    start_term,
    first_term,
    second_term,
    first_table,
    second_table,
    third_table,
    last_table,
    line_turns,
    base,
    target,
    sent_one,
    got_one,
    sent_two,
    got_two,
    sent_three,
    got_three,
    sent_four,
    got_four,
    lines_high,
    lines_low,
    lines_full,
    lines_imag,
    points,
    table_high,
    table_low,
    back_high,
    back_low,
    weight_last,
    send_sems,
    recv_sems,
):
    row, col = lax.axis_index("row"), lax.axis_index("col")
    own = col * ROWS + row
    lower_half = row < KEPT // 2
    holds = (col < LINES) & (lower_half | (row >= ROWS - KEPT // 2))
    kept_row = jnp.where(lower_half, row, jnp.where(row >= ROWS - KEPT // 2, row - 4, 0))
    kept_col = jnp.where(col < LINES, col, 0)

    def copy(source, destination, phase, peer_row, peer_col):
        return pltpu.make_async_remote_copy(
            source,
            destination,
            send_sems.at[phase],
            recv_sems.at[phase],
            device_id={"row": peer_row, "col": peer_col},
            device_id_type=pl.DeviceIdType.MESH,
        )

    def await_bytes(ref, sems, phase):
        pltpu.make_async_copy(ref, ref, sems.at[phase]).wait()

    def shuffle(group, carry):
        for part in range(2):
            for quarter in range(4):
                start = pl.multiple_of(group * 64, 64) + (part * 4 + quarter)
                sent_one[pl.ds(start, 8, stride=8), :] = section_field[
                    part,
                    pl.ds(pl.multiple_of(group * 8, 8), 8),
                    quarter * 128 : quarter * 128 + 128,
                ]
        return carry

    @pl.when(holds)
    def _():
        lax.fori_loop(0, BLOCK_X // 8, shuffle, 0)

        def send(step, carry):
            peer_row = lax.rem(row + step % ROWS, ROWS)
            peer_col = lax.rem(col + step // ROWS, COLS)
            copy(
                sent_one.at[pl.ds(pl.multiple_of((peer_col * ROWS + peer_row) * 8, 8), 8)],
                got_one.at[kept_col, pl.ds(pl.multiple_of(kept_row * 8, 8), 8)],
                0,
                peer_row,
                peer_col,
            ).start()
            return carry

        lax.fori_loop(1, DEVICES, send, 0)
        pltpu.make_async_copy(
            sent_one.at[pl.ds(pl.multiple_of(own * 8, 8), 8)],
            got_one.at[kept_col, pl.ds(pl.multiple_of(kept_row * 8, 8), 8)],
            recv_sems.at[0],
        ).start()

    def turn_tables(flip):
        high, low = (back_high, back_low) if flip else (table_high, table_low)

        def step(index, carry):
            cosine, sine = carry
            for place, value in enumerate((cosine, sine)):
                top, rest = split(value)
                if flip:
                    high[index, 128 * place : 128 * place + 128, :] = top
                    low[index, 128 * place : 128 * place + 128, :] = rest
                else:
                    high[index, :, 128 * place : 128 * place + 128] = top
                    low[index, :, 128 * place : 128 * place + 128] = rest
            spin_cos, spin_sin = base[2 + 2 * flip], base[3 + 2 * flip]
            return (
                cosine * spin_cos - sine * spin_sin,
                cosine * spin_sin + sine * spin_cos,
            )

        lax.fori_loop(0, PAIRS, step, (base[0], base[1]))

    turn_tables(0)

    await_bytes(got_one, recv_sems, 0)

    def wave_of(rows_shape):
        rows = lax.broadcasted_iota(jnp.int32, rows_shape, 0)
        lanes = lax.broadcasted_iota(jnp.int32, rows_shape, 1)
        block = lax.shift_right_logical(rows, 3)
        block = jnp.where(block < KEPT // 2, block, block + (ROWS - KEPT))
        index_y = block * BLOCK_Y + lax.bitwise_and(rows, 3) * 128 + lanes
        return jnp.where(index_y < LENGTH // 2, index_y, index_y - LENGTH)

    wave_y = wave_of((KEPT * 8, 128))
    kappa_y = wave_scale * wave_y.astype(FULL) / LENGTH
    keep_y = 3 * jnp.abs(wave_y) < LENGTH
    turn_cos = jnp.concatenate([line_turns[0], line_turns[0]], axis=1)
    turn_sin = jnp.concatenate([line_turns[1], line_turns[1]], axis=1)

    def line_in(l, carry):
        wave_x = l * BLOCK_X + own
        full_x = jnp.full((1, 128), wave_x, jnp.int32)
        kappa_x = wave_scale * full_x.astype(FULL) / LENGTH
        square = full_x * full_x + wave_y * wave_y
        inverse_sq = LENGTH * LENGTH / (9.0 * jnp.maximum(square, 1).astype(FULL))
        doubled = jnp.where(full_x == 0, 1.0, 2.0) * (1.0 / LENGTH)
        keep = keep_y & (3 * full_x < LENGTH)
        factor = jnp.where(keep, inverse_sq * doubled, 0.0)
        data = got_one[l]
        both = jnp.concatenate(
            [kappa_y * factor * data, -(kappa_x * factor) * data], axis=1
        )
        high, low = split(both)
        mixed = times(first_table[0], first_table[1], high, low)
        real, imag = mixed[:64], mixed[64:]
        out_real = real * turn_cos - imag * turn_sin
        out_imag = real * turn_sin + imag * turn_cos
        top, rest = split(jnp.concatenate([out_real, out_imag], axis=1))
        place = pl.ds(pl.multiple_of(l * 64, 64), 64)
        lines_high[place, :] = top
        lines_low[place, :] = rest
        return carry

    lax.fori_loop(0, LINES, line_in, 0)

    for quarter in range(4):
        if quarter % 2 == 0:
            wide = slice(128 * quarter, 128 * quarter + 256)
            lines_full[...] = times(
                lines_high[...],
                lines_low[...],
                second_table[0, :, wide],
                second_table[1, :, wide],
            )
        inner = slice(128 * (quarter % 2), 128 * (quarter % 2) + 128)

        def place_line(l, carry):
            for group in range(8):
                sent_two[
                    pl.ds((quarter * 64 + group * 8) * LINES + l, 8, stride=LINES), :
                ] = lines_full[
                    pl.ds(pl.multiple_of(l * 64, 64) + group * 8, 8), inner
                ]
            return carry

        lax.fori_loop(0, LINES, place_line, 0)

    def exchange(source, destination, phase):
        def send(step, carry):
            peer_row = lax.rem(row + step % ROWS, ROWS)
            peer_col = lax.rem(col + step // ROWS, COLS)
            copy(
                source.at[pl.ds((peer_col * ROWS + peer_row) * LINES, LINES)],
                destination.at[pl.ds(own * LINES, LINES)],
                phase,
                peer_row,
                peer_col,
            ).start()
            return carry

        lax.fori_loop(1, DEVICES, send, 0)
        pltpu.make_async_copy(
            source.at[pl.ds(own * LINES, LINES)],
            destination.at[pl.ds(own * LINES, LINES)],
            recv_sems.at[phase],
        ).start()

    exchange(sent_two, got_two, 1)

    def linear(group, carry):
        place = pl.ds(pl.multiple_of(group * 8, 8), 8)
        shape = (8, BLOCK_Y)
        wave_x = col * BLOCK_X + group * 8 + lax.broadcasted_iota(jnp.int32, shape, 0)
        index_y = row * BLOCK_Y + lax.broadcasted_iota(jnp.int32, shape, 1)
        signed_y = jnp.where(index_y < LENGTH // 2, index_y, index_y - LENGTH)
        damping, weight_a, weight_b, weight_c = section_weights(wave_x, signed_y)
        weight_last[place, :] = weight_c
        for part in range(2):
            target[part, place, :] = (
                damping * start_field[part, place, :]
                + weight_a * start_term[part, place, :]
                + 2.0 * weight_b * (first_term[part, place, :] + second_term[part, place, :])
            )
        return carry

    lax.fori_loop(0, BLOCK_X // 8, linear, 0)
    turn_tables(1)

    await_bytes(got_two, recv_sems, 1)

    lane = lax.broadcasted_iota(jnp.int32, (8, 128), 1)
    upper = lane >= 64

    def columns_in(group, carry):
        spread = []
        for high_bit in range(2):
            start = (high_bit * 128 + group * 8) * LINES
            spread.append(
                spread_lines(
                    [got_two[pl.ds(start + l, 8, stride=LINES), :] for l in range(LINES)],
                    upper,
                )
            )
        column = [None] * 64
        for step in range(32):
            other = spread[1][step]
            moved = total(
                [
                    scaled(cosine_of(step, 64), other),
                    scaled(sine_of(step, 64), turned(other, upper)) if step else None,
                ]
            )
            column[step] = spread[0][step] + moved
            column[step + 32] = spread[0][step] - moved
        place = pl.multiple_of(group * 8, 8)
        for step in range(PAIRS):
            value = column[step]
            if step % 32 == 0:
                real_part = jnp.where(upper, 0.0, value)
                imag_part = jnp.where(upper, 0.0, pltpu.roll(value, 64, 1))
            else:
                mirror = column[64 - step]
                real_part = jnp.where(upper, pltpu.roll(mirror, 64, 1), value)
                imag_part = jnp.where(upper, -mirror, pltpu.roll(value, 64, 1))
            points[step, pl.ds(place, 8), :] = real_part
            points[step, pl.ds(place + 128, 8), :] = imag_part
        return carry

    lax.fori_loop(0, 16, columns_in, 0)

    first_field = lax.broadcasted_iota(jnp.int32, (128, 128), 1) % 64 < 32

    def column_products(index, carry):
        high, low = split(points[index])
        grid = times(table_high[index], table_low[index], high, low)
        from_left = pltpu.roll(grid, 32, 1)
        from_right = pltpu.roll(grid, 96, 1)
        product = jnp.where(
            first_field, grid * from_right, (grid - from_left) * (grid + from_left)
        )
        high, low = split(product)
        points[index] = times(back_high[index], back_low[index], high, low)
        return carry

    lax.fori_loop(0, PAIRS, column_products, 0)

    def columns_out(group, carry):
        place = pl.multiple_of(group * 8, 8)
        column = [None] * 64
        for step in range(PAIRS):
            real_part = points[step, pl.ds(place, 8), :]
            imag_part = points[step, pl.ds(place + 128, 8), :]
            column[step] = jnp.where(upper, pltpu.roll(imag_part, 64, 1), real_part)
            if step % 32:
                column[64 - step] = jnp.where(
                    upper, -imag_part, pltpu.roll(real_part, 64, 1)
                )
        sums, gaps = [], []
        for step in range(32):
            sums.append(column[step] + column[step + 32])
            gap = column[step] - column[step + 32]
            gaps.append(
                total(
                    [
                        scaled(cosine_of(step, 64), gap),
                        scaled(-sine_of(step, 64), turned(gap, upper)) if step else None,
                    ]
                )
            )
        for high_bit, values in enumerate((sums, gaps)):
            start = (high_bit * 128 + group * 8) * LINES
            for l, value in enumerate(gather_lines(values, upper)):
                sent_three[pl.ds(start + l, 8, stride=LINES), :] = value
        return carry

    lax.fori_loop(0, 16, columns_out, 0)

    exchange(sent_three, got_three, 2)
    await_bytes(got_three, recv_sems, 2)

    def collect(l, carry):
        for quarter in range(4):
            for group in range(4):
                start = (quarter * 64 + group * 16) * LINES + l
                top, rest = split(
                    jnp.concatenate(
                        [
                            got_three[pl.ds(start, 8, stride=LINES), :],
                            got_three[pl.ds(start + 8 * LINES, 8, stride=LINES), :],
                        ]
                    )
                )
                place = pl.ds(pl.multiple_of(l * 64, 64) + group * 16, 16)
                lanes = slice(quarter * 128, quarter * 128 + 128)
                lines_high[place, lanes] = top
                lines_low[place, lanes] = rest
        return carry

    lax.fori_loop(0, LINES, collect, 0)

    for part, full in enumerate((lines_full, lines_imag)):
        wide = slice(256 * part, 256 * part + 256)
        full[...] = times(
            lines_high[...], lines_low[...], third_table[0, :, wide], third_table[1, :, wide]
        )

    def line_out(l, carry):
        place = pl.ds(pl.multiple_of(l * 64, 64), 64)
        real, imag = lines_full[place, :], lines_imag[place, :]
        out_real = real * turn_cos + imag * turn_sin
        out_imag = imag * turn_cos - real * turn_sin
        high, low = split(jnp.concatenate([out_real, out_imag], axis=0))
        value = times(last_table[0], last_table[1], high, low)
        full_x = jnp.full((1, 128), l * BLOCK_X + own, jnp.int32)
        kappa_x = wave_scale * full_x.astype(FULL) / LENGTH
        scale = jnp.where(keep_y & (3 * full_x < LENGTH), 1.0 / LENGTH, 0.0)
        weight_cross = (kappa_x * kappa_x - kappa_y * kappa_y) * scale
        weight_gap = kappa_x * kappa_y * scale
        sent_four[l] = weight_cross * value[:, :128] + weight_gap * value[:, 128:]
        return carry

    lax.fori_loop(0, LINES, line_out, 0)

    def send_term(step, carry):
        peer_col = lax.rem(kept_col + step // KEPT, LINES)
        block = lax.rem(kept_row + step % KEPT, KEPT)
        peer_row = jnp.where(block < KEPT // 2, block, block + (ROWS - KEPT))
        block_rows = pl.ds(pl.multiple_of(block * 8, 8), 8)
        target_rows = pl.ds(pl.multiple_of(own * 8, 8), 8)
        itself = (peer_row == row) & (peer_col == col)

        @pl.when(itself)
        def _():
            pltpu.make_async_copy(
                sent_four.at[peer_col, block_rows], got_four.at[target_rows], recv_sems.at[3]
            ).start()

        @pl.when(jnp.logical_not(itself))
        def _():
            copy(
                sent_four.at[peer_col, block_rows],
                got_four.at[target_rows],
                3,
                peer_row,
                peer_col,
            ).start()

        return carry

    lax.fori_loop(0, LINES * KEPT, send_term, 0)

    @pl.when(holds)
    def _():
        await_bytes(got_four, recv_sems, 3)

        def finish(group, carry):
            place = pl.ds(pl.multiple_of(group * 8, 8), 8)
            for part in range(2):
                for quarter in range(4):
                    lanes = slice(quarter * 128, quarter * 128 + 128)
                    start = pl.multiple_of(group * 64, 64) + (part * 4 + quarter)
                    target[part, place, lanes] = (
                        target[part, place, lanes]
                        + weight_last[place, lanes] * got_four[pl.ds(start, 8, stride=8), :]
                    )
            return carry

        lax.fori_loop(0, BLOCK_X // 8, finish, 0)
        others = sent_one.at[pl.ds(0, (DEVICES - 1) * 8)]
        await_bytes(others, send_sems, 0)
        await_bytes(sent_four.at[0, pl.ds(0, KEPT * 8 - 8)], send_sems, 3)
        await_bytes(sent_four.at[pl.ds(0, LINES - 1)], send_sems, 3)

    @pl.when(jnp.logical_not(holds))
    def _():
        await_bytes(sent_four, send_sems, 3)

    for phase, sent in ((1, sent_two), (2, sent_three)):
        await_bytes(sent.at[pl.ds(0, (DEVICES - 1) * LINES)], send_sems, phase)


def per_device(start_field, section_field, start_term, first_term, second_term):
    shape = (2, BLOCK_X, BLOCK_Y)
    fields = [
        field.reshape(shape)
        for field in (start_field, section_field, start_term, first_term, second_term)
    ]
    constants = [jnp.asarray(table) for table in tables()]
    vmem = pl.BlockSpec(memory_space=pltpu.VMEM)
    result = pl.pallas_call(
        section_kernel,
        out_shape=jax.ShapeDtypeStruct(shape, FULL),
        in_specs=[vmem] * (len(fields) + len(constants)),
        out_specs=vmem,
        scratch_shapes=[
            pltpu.VMEM((BLOCK_X * 8, 128), FULL),
            pltpu.VMEM((LINES, KEPT * 8, 128), FULL),
            pltpu.VMEM((DEVICES * LINES, 128), FULL),
            pltpu.VMEM((DEVICES * LINES, 128), FULL),
            pltpu.VMEM((DEVICES * LINES, 128), FULL),
            pltpu.VMEM((DEVICES * LINES, 128), FULL),
            pltpu.VMEM((LINES, KEPT * 8, 128), FULL),
            pltpu.VMEM((BLOCK_X * 8, 128), FULL),
            pltpu.VMEM((LINES * 64, 512), HIGH),
            pltpu.VMEM((LINES * 64, 512), HIGH),
            pltpu.VMEM((LINES * 64, 256), FULL),
            pltpu.VMEM((LINES * 64, 256), FULL),
            pltpu.VMEM((PAIRS, 256, 128), FULL),
            pltpu.VMEM((PAIRS, 128, 256), HIGH),
            pltpu.VMEM((PAIRS, 128, 256), HIGH),
            pltpu.VMEM((PAIRS, 256, 128), HIGH),
            pltpu.VMEM((PAIRS, 256, 128), HIGH),
            pltpu.VMEM((BLOCK_X, BLOCK_Y), FULL),
            pltpu.SemaphoreType.DMA((4,)),
            pltpu.SemaphoreType.DMA((4,)),
        ],
        compiler_params=pltpu.CompilerParams(
            has_side_effects=True, vmem_limit_bytes=56 * 2**20
        ),
        name="section",
    )(*fields, *constants)
    return result.reshape((1,) + shape)


def solution(mesh):
    spec = P(None, None, "col", "row")
    return jax.shard_map(
        per_device,
        mesh=mesh,
        in_specs=(spec,) * 5,
        out_specs=spec,
        check_vma=False,
    )
```

```python
import functools
import math

import jax
import jax.numpy as jnp
import ml_dtypes
import numpy as np
from jax import lax
from jax.experimental import pallas as pl
from jax.experimental.pallas import tpu as pltpu
from jax.sharding import PartitionSpec as P

LENGTH = 8192
ROWS = 16
COLS = 16
DEVICES = ROWS * COLS
BLOCK_X = 256
BLOCK_Y = 512
LINES = 11
KEPT = 12
PAIRS = 33

viscous_rate = 1.5
wave_scale = 3.0
series_terms = 12

HIGH = jnp.bfloat16
FULL = jnp.float32


def section_weights(wave_x, wave_y):
    square = wave_x * wave_x + wave_y * wave_y
    kappa_x = wave_scale * wave_x.astype(FULL) / LENGTH
    kappa_y = wave_scale * wave_y.astype(FULL) / LENGTH
    kappa_sq = kappa_x * kappa_x + kappa_y * kappa_y
    zvalue = -viscous_rate * kappa_sq
    damping = jnp.exp(zvalue)
    near_zero = 27 * square < 2 * LENGTH * LENGTH

    def series(degree):
        running = jnp.full_like(zvalue, 1.0 / math.factorial(series_terms - 1 + degree))
        for term_index in range(series_terms - 2, -1, -1):
            running = running * zvalue + 1.0 / math.factorial(term_index + degree)
        return running

    clamped = jnp.where(near_zero, -1.0, zvalue)
    exp_clamped = jnp.exp(clamped)
    closed_one = (exp_clamped - 1.0) / clamped
    closed_two = (exp_clamped - 1.0 - clamped) / (clamped * clamped)
    closed_three = (exp_clamped - 1.0 - clamped - 0.5 * clamped * clamped) / (
        clamped * clamped * clamped
    )
    phi_one = jnp.where(near_zero, series(1), closed_one)
    phi_two = jnp.where(near_zero, series(2), closed_two)
    phi_three = jnp.where(near_zero, series(3), closed_three)
    weight_a = phi_one - 3.0 * phi_two + 4.0 * phi_three
    weight_b = phi_two - 2.0 * phi_three
    weight_c = 4.0 * phi_three - phi_two
    return damping, weight_a, weight_b, weight_c


def halves(table):
    table = np.asarray(table, np.float32)
    high = table.astype(ml_dtypes.bfloat16)
    low = (table - high.astype(np.float32)).astype(ml_dtypes.bfloat16)
    return np.stack([high, low])


@functools.lru_cache(None)
def tables():
    row = np.arange(KEPT * 8)
    kept_row = row // 8
    source_row = np.where(kept_row < KEPT // 2, kept_row, kept_row + ROWS - KEPT)
    part = row % 8 // 4
    index_a = 4 * source_row + row % 4
    index_c = np.arange(64)
    angle = 2 * np.pi / 64 * (index_c[:, None] * index_a[None, :] % 64)
    cosine, sine = np.cos(angle), np.sin(angle)
    real_rows = np.where(part == 0, -sine, -cosine)
    imag_rows = np.where(part == 0, cosine, -sine)
    first = np.concatenate([real_rows, imag_rows])
    real_out = np.where(part == 0, cosine, -sine)
    imag_out = np.where(part == 0, sine, cosine)
    last = np.concatenate([real_out, imag_out]).T
    index_b = np.arange(128)
    turn = 2 * np.pi / LENGTH * (index_c[:, None] * index_b[None, :])
    turns = np.stack([np.cos(turn), np.sin(turn)]).astype(np.float32)
    angle = 2 * np.pi / 128 * (index_b[:, None] * index_b[None, :] % 128)
    cosine, sine = np.cos(angle), np.sin(angle)
    second = np.zeros((2, 2, 128, 4, 2, 2, 32))
    for field in range(2):
        second[0, field, :, :, 0, field] = cosine.reshape(128, 4, 32)
        second[0, field, :, :, 1, field] = sine.reshape(128, 4, 32)
        second[1, field, :, :, 0, field] = -sine.reshape(128, 4, 32)
        second[1, field, :, :, 1, field] = cosine.reshape(128, 4, 32)
    second = second.reshape(512, 512)
    spin = 2 * np.pi / LENGTH * np.broadcast_to(index_b[None, :], (128, 128))
    base = np.stack(
        [cosine, -sine, np.cos(spin), -np.sin(spin), np.cos(spin.T), -np.sin(spin.T)]
    ).astype(np.float32)
    wide = np.stack(
        [np.concatenate(halves(second[:, 128 * g : 128 * g + 128]), axis=1) for g in range(4)]
    )
    return halves(first), wide, halves(second.T), halves(last), turns, base


def split(values):
    high = values.astype(HIGH)
    return high, (values - high.astype(FULL)).astype(HIGH)


def times(left_high, left_low, right_high, right_low):
    dot = functools.partial(jnp.dot, preferred_element_type=FULL)
    return (
        dot(left_high, right_low) + dot(left_low, right_high)
    ) + dot(left_high, right_high)


def turned(values, upper):
    moved = pltpu.roll(values, 64, 1)
    return jnp.where(upper, moved, -moved)


def cosine_of(step, period):
    return math.cos(2 * math.pi * (step % period) / period)


def sine_of(step, period):
    return math.sin(2 * math.pi * (step % period) / period)


def scaled(factor, value):
    if abs(factor) < 1e-12:
        return None
    if abs(factor - 1) < 1e-12:
        return value
    if abs(factor + 1) < 1e-12:
        return -value
    return factor * value


def total(values):
    values = [value for value in values if value is not None]
    if not values:
        return None
    return functools.reduce(lambda a, b: a + b, values)


def plus(a, b):
    return b if a is None else a if b is None else a + b


def minus(a, b):
    return a if b is None else -b if a is None else a - b


def spread_lines(lines, upper):
    turns = [turned(line, upper) for line in lines]
    out = [None] * 32
    for step in range(9):
        sums = []
        for parity in range(2):
            picked = range(parity, LINES, 2)
            sums.append(total(scaled(cosine_of(l * step, 32), lines[l]) for l in picked))
            sums.append(total(scaled(sine_of(l * step, 32), turns[l]) for l in picked))
        cos_even, sin_even, cos_odd, sin_odd = sums
        cos_sum, cos_gap = plus(cos_even, cos_odd), minus(cos_even, cos_odd)
        sin_sum, sin_gap = plus(sin_even, sin_odd), minus(sin_even, sin_odd)
        out[step] = plus(cos_sum, sin_sum)
        out[(16 + step) % 32] = plus(cos_gap, sin_gap)
        if step:
            out[32 - step] = minus(cos_sum, sin_sum)
            out[16 - step] = minus(cos_gap, sin_gap)
    return out


def gather_lines(points, upper):
    out = [None] * LINES
    for parity in range(2):
        sign = 1 - 2 * parity
        folded = [
            points[step] + points[step + 16] if sign > 0 else points[step] - points[step + 16]
            for step in range(16)
        ]
        even, odd = [folded[0]], [None]
        for step in range(1, 8):
            mirror = folded[16 - step]
            even.append(folded[step] + mirror if sign > 0 else folded[step] - mirror)
            odd.append(
                turned(folded[step] - mirror if sign > 0 else folded[step] + mirror, upper)
            )
        even.append(folded[8])
        odd.append(turned(folded[8], upper))
        for l in range(parity, LINES, 2):
            terms = [scaled(cosine_of(l * step, 32), even[step]) for step in range(9)]
            terms += [scaled(-sine_of(l * step, 32), odd[step]) for step in range(1, 9)]
            out[l] = total(terms)
    return out


def section_kernel(
    start_field,
    section_field,
    start_term,
    first_term,
    second_term,
    first_table,
    second_table,
    third_table,
    last_table,
    line_turns,
    base,
    target,
    sent_one,
    got_one,
    sent_two,
    got_two,
    sent_three,
    got_three,
    sent_four,
    got_four,
    lines_high,
    lines_low,
    lines_full,
    lines_imag,
    points,
    table,
    back,
    weight_last,
    send_sems,
    recv_sems,
    line_sems,
    column_sems,
):
    row, col = lax.axis_index("row"), lax.axis_index("col")
    own = col * ROWS + row
    own_line = col * 8 + lax.rem(row, 8) + 128 * (row // 8)
    lower_half = row < KEPT // 2
    holds = (col < LINES) & (lower_half | (row >= ROWS - KEPT // 2))
    kept_row = jnp.where(lower_half, row, jnp.where(row >= ROWS - KEPT // 2, row - 4, 0))
    kept_col = jnp.where(col < LINES, col, 0)

    def post(source, destination, phase, peer_row, peer_col, sem):
        itself = (peer_row == row) & (peer_col == col)

        @pl.when(itself)
        def _():
            pltpu.make_async_copy(source, destination, sem).start()

        @pl.when(jnp.logical_not(itself))
        def _():
            pltpu.make_async_remote_copy(
                source,
                destination,
                send_sems.at[phase],
                sem,
                device_id={"row": peer_row, "col": peer_col},
                device_id_type=pl.DeviceIdType.MESH,
            ).start()

    def await_bytes(ref, sem):
        pltpu.make_async_copy(ref, ref, sem).wait()

    def shuffle(group, carry):
        for part in range(2):
            for quarter in range(4):
                start = pl.multiple_of(group * 64, 64) + (part * 4 + quarter)
                sent_one[pl.ds(start, 8, stride=8), :] = section_field[
                    part,
                    pl.ds(pl.multiple_of(group * 8, 8), 8),
                    quarter * 128 : quarter * 128 + 128,
                ]
        return carry

    @pl.when(holds)
    def _():
        lax.fori_loop(0, BLOCK_X // 8, shuffle, 0)

        def send(step, carry):
            peer_row = lax.rem(row + step % ROWS, ROWS)
            peer_col = lax.rem(col + step // ROWS, COLS)
            line = peer_col * 8 + lax.rem(peer_row, 8) + 128 * (peer_row // 8)
            post(
                sent_one.at[pl.ds(pl.multiple_of(line * 8, 8), 8)],
                got_one.at[kept_col, pl.ds(pl.multiple_of(kept_row * 8, 8), 8)],
                0,
                peer_row,
                peer_col,
                line_sems.at[kept_col],
            )
            return carry

        lax.fori_loop(0, DEVICES, send, 0)

    def turn_tables(flip):
        def step(index, carry):
            cosine, sine = carry
            for place, value in enumerate((cosine, sine)):
                top, rest = split(value)
                span = slice(128 * place, 128 * place + 128)
                if flip:
                    back[index, span, 0:128] = top
                    back[index, span, 128:256] = rest
                else:
                    table[index, 0:128, span] = top
                    table[index, 128:256, span] = rest
            spin_cos, spin_sin = base[2 + 2 * flip], base[3 + 2 * flip]
            return (
                cosine * spin_cos - sine * spin_sin,
                cosine * spin_sin + sine * spin_cos,
            )

        lax.fori_loop(0, PAIRS, step, (base[0], base[1]))

    turn_tables(0)

    def wave_of(rows_shape):
        rows = lax.broadcasted_iota(jnp.int32, rows_shape, 0)
        lanes = lax.broadcasted_iota(jnp.int32, rows_shape, 1)
        block = lax.shift_right_logical(rows, 3)
        block = jnp.where(block < KEPT // 2, block, block + (ROWS - KEPT))
        index_y = block * BLOCK_Y + lax.bitwise_and(rows, 3) * 128 + lanes
        return jnp.where(index_y < LENGTH // 2, index_y, index_y - LENGTH)

    wave_y = wave_of((KEPT * 8, 128))
    kappa_y = wave_scale * wave_y.astype(FULL) / LENGTH
    keep_y = 3 * jnp.abs(wave_y) < LENGTH
    turn_cos = jnp.concatenate([line_turns[0], line_turns[0]], axis=1)
    turn_sin = jnp.concatenate([line_turns[1], line_turns[1]], axis=1)

    def line_in(l):
        await_bytes(got_one.at[l], line_sems.at[l])
        wave_x = l * BLOCK_X + own_line
        full_x = jnp.full((1, 128), wave_x, jnp.int32)
        kappa_x = wave_scale * full_x.astype(FULL) / LENGTH
        square = full_x * full_x + wave_y * wave_y
        inverse_sq = LENGTH * LENGTH / (9.0 * jnp.maximum(square, 1).astype(FULL))
        doubled = jnp.where(full_x == 0, 1.0, 2.0) * (1.0 / LENGTH)
        keep = keep_y & (3 * full_x < LENGTH)
        factor = jnp.where(keep, inverse_sq * doubled, 0.0)
        data = got_one[l]
        both = jnp.concatenate(
            [kappa_y * factor * data, -(kappa_x * factor) * data], axis=1
        )
        high, low = split(both)
        mixed = times(first_table[0], first_table[1], high, low)
        real, imag = mixed[:64], mixed[64:]
        out_real = real * turn_cos - imag * turn_sin
        out_imag = real * turn_sin + imag * turn_cos
        top, rest = split(jnp.concatenate([out_real, out_imag], axis=1))
        place = pl.ds(pl.multiple_of(l * 64, 64), 64)
        lines_high[place, :] = top
        lines_low[place, :] = rest

    def line_step(step, carry):
        l = lax.rem(col + COLS - step, COLS)

        @pl.when(l < LINES)
        def _():
            line_in(l)

        return carry

    lax.fori_loop(0, COLS, line_step, 0)

    def post_column(source, destination, phase, peer_col, sem):
        def send(step, carry):
            peer_row = lax.rem(row + step, ROWS)
            post(
                source.at[pl.ds((peer_col * ROWS + peer_row) * LINES, LINES)],
                destination.at[pl.ds(own * LINES, LINES)],
                phase,
                peer_row,
                peer_col,
                sem,
            )
            return carry

        lax.fori_loop(0, ROWS, send, 0)

    def quarter_out(step, carry):
        quarter = lax.rem(col // 4 + step, 4)
        high_part = jnp.dot(lines_high[...], second_table[quarter], preferred_element_type=FULL)
        low_part = jnp.dot(
            lines_low[...], second_table[quarter, :, 0:128], preferred_element_type=FULL
        )
        lines_full[:, 0:128] = (high_part[:, 128:256] + low_part) + high_part[:, 0:128]

        def place_line(l, inner):
            for group in range(8):
                sent_two[
                    pl.ds((quarter * 64 + group * 8) * LINES + l, 8, stride=LINES), :
                ] = lines_full[pl.ds(pl.multiple_of(l * 64, 64) + group * 8, 8), 0:128]
            return inner

        lax.fori_loop(0, LINES, place_line, 0)

        def send_quarter(offset, inner):
            peer_col = quarter * 4 + lax.rem(col + offset, 4)
            post_column(sent_two, got_two, 1, peer_col, column_sems.at[col])
            return inner

        lax.fori_loop(0, 4, send_quarter, 0)
        return carry

    lax.fori_loop(0, 4, quarter_out, 0)

    def linear(group, carry):
        place = pl.ds(pl.multiple_of(group * 8, 8), 8)
        shape = (8, BLOCK_Y)
        wave_x = col * BLOCK_X + group * 8 + lax.broadcasted_iota(jnp.int32, shape, 0)
        index_y = row * BLOCK_Y + lax.broadcasted_iota(jnp.int32, shape, 1)
        signed_y = jnp.where(index_y < LENGTH // 2, index_y, index_y - LENGTH)
        damping, weight_a, weight_b, weight_c = section_weights(wave_x, signed_y)
        weight_last[place, :] = weight_c
        for part in range(2):
            target[part, place, :] = (
                damping * start_field[part, place, :]
                + weight_a * start_term[part, place, :]
                + 2.0 * weight_b * (first_term[part, place, :] + second_term[part, place, :])
            )
        return carry

    lax.fori_loop(0, BLOCK_X // 8, linear, 0)
    turn_tables(1)

    lane = lax.broadcasted_iota(jnp.int32, (8, 128), 1)
    upper = lane >= 64

    def columns_in(step_in, carry):
        group = 4 * lax.rem(col // 4 + 4 - step_in // 4, 4) + lax.rem(
            col + 4 - step_in % 4, 4
        )
        await_bytes(
            got_two.at[pl.ds(group * ROWS * LINES, ROWS * LINES)], column_sems.at[group]
        )
        spread = []
        for high_bit in range(2):
            start = (high_bit * 8 + group * 16) * LINES
            spread.append(
                spread_lines(
                    [got_two[pl.ds(start + l, 8, stride=LINES), :] for l in range(LINES)],
                    upper,
                )
            )
        column = [None] * 64
        for step in range(32):
            other = spread[1][step]
            moved = total(
                [
                    scaled(cosine_of(step, 64), other),
                    scaled(sine_of(step, 64), turned(other, upper)) if step else None,
                ]
            )
            column[step] = spread[0][step] + moved
            column[step + 32] = spread[0][step] - moved
        place = pl.multiple_of(group * 8, 8)
        for step in range(PAIRS):
            value = column[step]
            if step % 32 == 0:
                real_part = jnp.where(upper, 0.0, value)
                imag_part = jnp.where(upper, 0.0, pltpu.roll(value, 64, 1))
            else:
                mirror = column[64 - step]
                real_part = jnp.where(upper, pltpu.roll(mirror, 64, 1), value)
                imag_part = jnp.where(upper, -mirror, pltpu.roll(value, 64, 1))
            points[step, pl.ds(place, 8), :] = real_part
            points[step, pl.ds(place + 128, 8), :] = imag_part
        return carry

    lax.fori_loop(0, 16, columns_in, 0)

    first_field = lax.broadcasted_iota(jnp.int32, (128, 128), 1) % 64 < 32

    def column_products(step, carry):
        for index in (3 * step, 3 * step + 1, 3 * step + 2):
            high, low = split(points[index])
            wide = jnp.dot(
                table[index],
                jnp.concatenate([high, low], axis=1),
                preferred_element_type=FULL,
            )
            grid = (wide[:128, 128:] + wide[128:, :128]) + wide[:128, :128]
            from_left = pltpu.roll(grid, 32, 1)
            from_right = pltpu.roll(grid, 96, 1)
            product = jnp.where(
                first_field, grid * from_right, (grid - from_left) * (grid + from_left)
            )
            both = jnp.concatenate(split(product), axis=1)
            wide = jnp.dot(
                back[index],
                jnp.concatenate([both, both], axis=0),
                preferred_element_type=FULL,
            )
            points[index] = wide[:, 128:] + wide[:, :128]
        return carry

    lax.fori_loop(0, PAIRS // 3, column_products, 0)

    def columns_out(step_out, carry):
        group = lax.rem(col + step_out, COLS)
        place = pl.multiple_of(group * 8, 8)
        column = [None] * 64
        for step in range(PAIRS):
            real_part = points[step, pl.ds(place, 8), :]
            imag_part = points[step, pl.ds(place + 128, 8), :]
            column[step] = jnp.where(upper, pltpu.roll(imag_part, 64, 1), real_part)
            if step % 32:
                column[64 - step] = jnp.where(
                    upper, -imag_part, pltpu.roll(real_part, 64, 1)
                )
        sums, gaps = [], []
        for step in range(32):
            sums.append(column[step] + column[step + 32])
            gap = column[step] - column[step + 32]
            gaps.append(
                total(
                    [
                        scaled(cosine_of(step, 64), gap),
                        scaled(-sine_of(step, 64), turned(gap, upper)) if step else None,
                    ]
                )
            )
        for high_bit, values in enumerate((sums, gaps)):
            start = (high_bit * 8 + group * 16) * LINES
            for l, value in enumerate(gather_lines(values, upper)):
                sent_three[pl.ds(start + l, 8, stride=LINES), :] = value
        post_column(sent_three, got_three, 2, group, recv_sems.at[0])
        return carry

    lax.fori_loop(0, 16, columns_out, 0)

    await_bytes(got_three, recv_sems.at[0])

    def collect(l, carry):
        for quarter in range(4):
            for group in range(4):
                start = (quarter * 64 + group * 16) * LINES + l
                top, rest = split(
                    jnp.concatenate(
                        [
                            got_three[pl.ds(start, 8, stride=LINES), :],
                            got_three[pl.ds(start + 8 * LINES, 8, stride=LINES), :],
                        ]
                    )
                )
                place = pl.ds(pl.multiple_of(l * 64, 64) + group * 16, 16)
                lanes = slice(quarter * 128, quarter * 128 + 128)
                lines_high[place, lanes] = top
                lines_low[place, lanes] = rest
        return carry

    lax.fori_loop(0, LINES, collect, 0)

    for part, full in enumerate((lines_full, lines_imag)):
        wide = slice(256 * part, 256 * part + 256)
        full[...] = times(
            lines_high[...], lines_low[...], third_table[0, :, wide], third_table[1, :, wide]
        )

    def line_out(step_out, carry):
        l = lax.rem(kept_col + step_out, LINES)
        place = pl.ds(pl.multiple_of(l * 64, 64), 64)
        real, imag = lines_full[place, :], lines_imag[place, :]
        out_real = real * turn_cos + imag * turn_sin
        out_imag = imag * turn_cos - real * turn_sin
        high, low = split(jnp.concatenate([out_real, out_imag], axis=0))
        value = times(last_table[0], last_table[1], high, low)
        full_x = jnp.full((1, 128), l * BLOCK_X + own_line, jnp.int32)
        kappa_x = wave_scale * full_x.astype(FULL) / LENGTH
        scale = jnp.where(keep_y & (3 * full_x < LENGTH), 1.0 / LENGTH, 0.0)
        weight_cross = (kappa_x * kappa_x - kappa_y * kappa_y) * scale
        weight_gap = kappa_x * kappa_y * scale
        sent_four[l] = weight_cross * value[:, :128] + weight_gap * value[:, 128:]

        def send_term(step, inner):
            block = lax.rem(kept_row + step, KEPT)
            post(
                sent_four.at[l, pl.ds(pl.multiple_of(block * 8, 8), 8)],
                got_four.at[pl.ds(pl.multiple_of(own_line * 8, 8), 8)],
                3,
                jnp.where(block < KEPT // 2, block, block + (ROWS - KEPT)),
                l,
                recv_sems.at[1],
            )
            return inner

        lax.fori_loop(0, KEPT, send_term, 0)
        return carry

    lax.fori_loop(0, LINES, line_out, 0)

    @pl.when(holds)
    def _():
        await_bytes(got_four, recv_sems.at[1])

        def finish(group, carry):
            place = pl.ds(pl.multiple_of(group * 8, 8), 8)
            for part in range(2):
                for quarter in range(4):
                    lanes = slice(quarter * 128, quarter * 128 + 128)
                    start = pl.multiple_of(group * 64, 64) + (part * 4 + quarter)
                    target[part, place, lanes] = (
                        target[part, place, lanes]
                        + weight_last[place, lanes] * got_four[pl.ds(start, 8, stride=8), :]
                    )
            return carry

        lax.fori_loop(0, BLOCK_X // 8, finish, 0)
        others = sent_one.at[pl.ds(0, (DEVICES - 1) * 8)]
        await_bytes(others, send_sems.at[0])
        await_bytes(sent_four.at[0, pl.ds(0, KEPT * 8 - 8)], send_sems.at[3])
        await_bytes(sent_four.at[pl.ds(0, LINES - 1)], send_sems.at[3])

    @pl.when(jnp.logical_not(holds))
    def _():
        await_bytes(sent_four, send_sems.at[3])

    for phase, sent in ((1, sent_two), (2, sent_three)):
        await_bytes(sent.at[pl.ds(0, (DEVICES - 1) * LINES)], send_sems.at[phase])


def per_device(start_field, section_field, start_term, first_term, second_term):
    shape = (2, BLOCK_X, BLOCK_Y)
    fields = [
        field.reshape(shape)
        for field in (start_field, section_field, start_term, first_term, second_term)
    ]
    constants = [jnp.asarray(table) for table in tables()]
    vmem = pl.BlockSpec(memory_space=pltpu.VMEM)
    result = pl.pallas_call(
        section_kernel,
        out_shape=jax.ShapeDtypeStruct(shape, FULL),
        in_specs=[vmem] * (len(fields) + len(constants)),
        out_specs=vmem,
        scratch_shapes=[
            pltpu.VMEM((BLOCK_X * 8, 128), FULL),
            pltpu.VMEM((LINES, KEPT * 8, 128), FULL),
            pltpu.VMEM((DEVICES * LINES, 128), FULL),
            pltpu.VMEM((DEVICES * LINES, 128), FULL),
            pltpu.VMEM((DEVICES * LINES, 128), FULL),
            pltpu.VMEM((DEVICES * LINES, 128), FULL),
            pltpu.VMEM((LINES, KEPT * 8, 128), FULL),
            pltpu.VMEM((BLOCK_X * 8, 128), FULL),
            pltpu.VMEM((LINES * 64, 512), HIGH),
            pltpu.VMEM((LINES * 64, 512), HIGH),
            pltpu.VMEM((LINES * 64, 256), FULL),
            pltpu.VMEM((LINES * 64, 256), FULL),
            pltpu.VMEM((PAIRS, 256, 128), FULL),
            pltpu.VMEM((PAIRS, 256, 256), HIGH),
            pltpu.VMEM((PAIRS, 256, 256), HIGH),
            pltpu.VMEM((BLOCK_X, BLOCK_Y), FULL),
            pltpu.SemaphoreType.DMA((4,)),
            pltpu.SemaphoreType.DMA((2,)),
            pltpu.SemaphoreType.DMA((LINES,)),
            pltpu.SemaphoreType.DMA((COLS,)),
        ],
        compiler_params=pltpu.CompilerParams(
            has_side_effects=True, vmem_limit_bytes=56 * 2**20
        ),
        name="section",
    )(*fields, *constants)
    return result.reshape((1,) + shape)


def solution(mesh):
    spec = P(None, None, "col", "row")
    return jax.shard_map(
        per_device,
        mesh=mesh,
        in_specs=(spec,) * 5,
        out_specs=spec,
        check_vma=False,
    )
```

```python
import functools
import math

import jax
import jax.numpy as jnp
import ml_dtypes
import numpy as np
from jax import lax
from jax.experimental import pallas as pl
from jax.experimental.pallas import tpu as pltpu
from jax.sharding import PartitionSpec as P

LENGTH = 8192
ROWS = 16
COLS = 16
DEVICES = ROWS * COLS
BLOCK_X = 256
BLOCK_Y = 512
LINES = 11
KEPT = 12
PAIRS = 33

viscous_rate = 1.5
wave_scale = 3.0
series_terms = 12

HIGH = jnp.bfloat16
FULL = jnp.float32


def section_weights(wave_x, wave_y):
    square = wave_x * wave_x + wave_y * wave_y
    kappa_x = wave_scale * wave_x.astype(FULL) / LENGTH
    kappa_y = wave_scale * wave_y.astype(FULL) / LENGTH
    kappa_sq = kappa_x * kappa_x + kappa_y * kappa_y
    zvalue = -viscous_rate * kappa_sq
    damping = jnp.exp(zvalue)
    near_zero = 27 * square < 2 * LENGTH * LENGTH

    def series(degree):
        running = jnp.full_like(zvalue, 1.0 / math.factorial(series_terms - 1 + degree))
        for term_index in range(series_terms - 2, -1, -1):
            running = running * zvalue + 1.0 / math.factorial(term_index + degree)
        return running

    clamped = jnp.where(near_zero, -1.0, zvalue)
    exp_clamped = jnp.exp(clamped)
    closed_one = (exp_clamped - 1.0) / clamped
    closed_two = (exp_clamped - 1.0 - clamped) / (clamped * clamped)
    closed_three = (exp_clamped - 1.0 - clamped - 0.5 * clamped * clamped) / (
        clamped * clamped * clamped
    )
    phi_one = jnp.where(near_zero, series(1), closed_one)
    phi_two = jnp.where(near_zero, series(2), closed_two)
    phi_three = jnp.where(near_zero, series(3), closed_three)
    weight_a = phi_one - 3.0 * phi_two + 4.0 * phi_three
    weight_b = phi_two - 2.0 * phi_three
    weight_c = 4.0 * phi_three - phi_two
    return damping, weight_a, weight_b, weight_c


def halves(table):
    table = np.asarray(table, np.float32)
    high = table.astype(ml_dtypes.bfloat16)
    low = (table - high.astype(np.float32)).astype(ml_dtypes.bfloat16)
    return np.stack([high, low])


@functools.lru_cache(None)
def tables():
    row = np.arange(KEPT * 8)
    kept_row = row // 8
    source_row = np.where(kept_row < KEPT // 2, kept_row, kept_row + ROWS - KEPT)
    part = row % 8 // 4
    index_a = 4 * source_row + row % 4
    index_c = np.arange(64)
    angle = 2 * np.pi / 64 * (index_c[:, None] * index_a[None, :] % 64)
    cosine, sine = np.cos(angle), np.sin(angle)
    real_rows = np.where(part == 0, -sine, -cosine)
    imag_rows = np.where(part == 0, cosine, -sine)
    first = np.concatenate([real_rows, imag_rows])
    real_out = np.where(part == 0, cosine, -sine)
    imag_out = np.where(part == 0, sine, cosine)
    last = np.concatenate([real_out, imag_out]).T
    index_b = np.arange(128)
    turn = 2 * np.pi / LENGTH * (index_c[:, None] * index_b[None, :])
    turns = np.stack([np.cos(turn), np.sin(turn)]).astype(np.float32)
    angle = 2 * np.pi / 128 * (index_b[:, None] * index_b[None, :] % 128)
    cosine, sine = np.cos(angle), np.sin(angle)
    second = np.zeros((2, 2, 128, 4, 2, 2, 32))
    for field in range(2):
        second[0, field, :, :, 0, field] = cosine.reshape(128, 4, 32)
        second[0, field, :, :, 1, field] = sine.reshape(128, 4, 32)
        second[1, field, :, :, 0, field] = -sine.reshape(128, 4, 32)
        second[1, field, :, :, 1, field] = cosine.reshape(128, 4, 32)
    second = second.reshape(512, 512)
    spin = 2 * np.pi / LENGTH * np.broadcast_to(index_b[None, :], (128, 128))
    base = np.stack(
        [cosine, -sine, np.cos(spin), -np.sin(spin), np.cos(spin.T), -np.sin(spin.T)]
    ).astype(np.float32)
    wide = np.stack(
        [np.concatenate(halves(second[:, 128 * g : 128 * g + 128]), axis=1) for g in range(4)]
    )
    return halves(first), wide, halves(second.T), halves(last), turns, base


def split(values):
    high = values.astype(HIGH)
    return high, (values - high.astype(FULL)).astype(HIGH)


def times(left_high, left_low, right_high, right_low):
    dot = functools.partial(jnp.dot, preferred_element_type=FULL)
    return (
        dot(left_high, right_low) + dot(left_low, right_high)
    ) + dot(left_high, right_high)


def turned(values, upper):
    moved = pltpu.roll(values, 64, 1)
    return jnp.where(upper, moved, -moved)


def cosine_of(step, period):
    return math.cos(2 * math.pi * (step % period) / period)


def sine_of(step, period):
    return math.sin(2 * math.pi * (step % period) / period)


def scaled(factor, value):
    if abs(factor) < 1e-12:
        return None
    if abs(factor - 1) < 1e-12:
        return value
    if abs(factor + 1) < 1e-12:
        return -value
    return factor * value


def total(values):
    values = [value for value in values if value is not None]
    if not values:
        return None
    return functools.reduce(lambda a, b: a + b, values)


def plus(a, b):
    return b if a is None else a if b is None else a + b


def minus(a, b):
    return a if b is None else -b if a is None else a - b


def spread_lines(lines, upper):
    turns = [turned(line, upper) for line in lines]
    out = [None] * 32
    for step in range(9):
        sums = []
        for parity in range(2):
            picked = range(parity, LINES, 2)
            sums.append(total(scaled(cosine_of(l * step, 32), lines[l]) for l in picked))
            sums.append(total(scaled(sine_of(l * step, 32), turns[l]) for l in picked))
        cos_even, sin_even, cos_odd, sin_odd = sums
        cos_sum, cos_gap = plus(cos_even, cos_odd), minus(cos_even, cos_odd)
        sin_sum, sin_gap = plus(sin_even, sin_odd), minus(sin_even, sin_odd)
        out[step] = plus(cos_sum, sin_sum)
        out[(16 + step) % 32] = plus(cos_gap, sin_gap)
        if step:
            out[32 - step] = minus(cos_sum, sin_sum)
            out[16 - step] = minus(cos_gap, sin_gap)
    return out


def gather_lines(points, upper):
    out = [None] * LINES
    for parity in range(2):
        sign = 1 - 2 * parity
        folded = [
            points[step] + points[step + 16] if sign > 0 else points[step] - points[step + 16]
            for step in range(16)
        ]
        even, odd = [folded[0]], [None]
        for step in range(1, 8):
            mirror = folded[16 - step]
            even.append(folded[step] + mirror if sign > 0 else folded[step] - mirror)
            odd.append(
                turned(folded[step] - mirror if sign > 0 else folded[step] + mirror, upper)
            )
        even.append(folded[8])
        odd.append(turned(folded[8], upper))
        for l in range(parity, LINES, 2):
            terms = [scaled(cosine_of(l * step, 32), even[step]) for step in range(9)]
            terms += [scaled(-sine_of(l * step, 32), odd[step]) for step in range(1, 9)]
            out[l] = total(terms)
    return out


def section_kernel(
    start_field,
    section_field,
    start_term,
    first_term,
    second_term,
    first_table,
    second_table,
    third_table,
    last_table,
    line_turns,
    base,
    target,
    sent_one,
    got_one,
    sent_two,
    got_two,
    sent_three,
    got_three,
    sent_four,
    got_four,
    lines_high,
    lines_low,
    lines_full,
    lines_imag,
    points,
    table,
    back,
    weight_last,
    send_sems,
    recv_sems,
    line_sems,
    column_sems,
):
    row, col = lax.axis_index("row"), lax.axis_index("col")
    own = col * ROWS + row
    own_line = col * 8 + lax.rem(row, 8) + 128 * (row // 8)
    lower_half = row < KEPT // 2
    holds = (col < LINES) & (lower_half | (row >= ROWS - KEPT // 2))
    kept_row = jnp.where(lower_half, row, jnp.where(row >= ROWS - KEPT // 2, row - 4, 0))
    kept_col = jnp.where(col < LINES, col, 0)

    def far_first(step):
        back_step = 3 - step
        return lax.bitwise_xor(back_step, lax.shift_right_logical(back_step, 1))

    def col_at(step, sign):
        across = lax.rem(col // 4 + 4 + sign * far_first(step // 4), 4)
        along = lax.rem(lax.rem(col, 4) + 4 + sign * far_first(lax.rem(step, 4)), 4)
        return 4 * across + along

    def row_at(step):
        across = lax.rem(row // 4 + far_first(step // 4), 4)
        return 4 * across + lax.bitwise_xor(lax.rem(row, 4), 3 - lax.rem(step, 4))

    def post(source, destination, phase, peer_row, peer_col, sem):
        itself = (peer_row == row) & (peer_col == col)

        @pl.when(itself)
        def _():
            pltpu.make_async_copy(source, destination, sem).start()

        @pl.when(jnp.logical_not(itself))
        def _():
            pltpu.make_async_remote_copy(
                source,
                destination,
                send_sems.at[phase],
                sem,
                device_id={"row": peer_row, "col": peer_col},
                device_id_type=pl.DeviceIdType.MESH,
            ).start()

    def await_bytes(ref, sem):
        pltpu.make_async_copy(ref, ref, sem).wait()

    def shuffle(group, carry):
        for part in range(2):
            for quarter in range(4):
                start = pl.multiple_of(group * 64, 64) + (part * 4 + quarter)
                sent_one[pl.ds(start, 8, stride=8), :] = section_field[
                    part,
                    pl.ds(pl.multiple_of(group * 8, 8), 8),
                    quarter * 128 : quarter * 128 + 128,
                ]
        return carry

    @pl.when(holds)
    def _():
        lax.fori_loop(0, BLOCK_X // 8, shuffle, 0)

        def send(step, carry):
            peer_row = row_at(lax.rem(step, ROWS))
            peer_col = col_at(step // ROWS, 1)
            line = peer_col * 8 + lax.rem(peer_row, 8) + 128 * (peer_row // 8)
            post(
                sent_one.at[pl.ds(pl.multiple_of(line * 8, 8), 8)],
                got_one.at[kept_col, pl.ds(pl.multiple_of(kept_row * 8, 8), 8)],
                0,
                peer_row,
                peer_col,
                line_sems.at[kept_col],
            )
            return carry

        lax.fori_loop(0, DEVICES, send, 0)

    def turn_tables(flip):
        def step(index, carry):
            cosine, sine = carry
            for place, value in enumerate((cosine, sine)):
                top, rest = split(value)
                span = slice(128 * place, 128 * place + 128)
                if flip:
                    back[index, span, 0:128] = top
                    back[index, span, 128:256] = rest
                else:
                    table[index, 0:128, span] = top
                    table[index, 128:256, span] = rest
            spin_cos, spin_sin = base[2 + 2 * flip], base[3 + 2 * flip]
            return (
                cosine * spin_cos - sine * spin_sin,
                cosine * spin_sin + sine * spin_cos,
            )

        lax.fori_loop(0, PAIRS, step, (base[0], base[1]))

    turn_tables(0)

    def wave_of(rows_shape):
        rows = lax.broadcasted_iota(jnp.int32, rows_shape, 0)
        lanes = lax.broadcasted_iota(jnp.int32, rows_shape, 1)
        block = lax.shift_right_logical(rows, 3)
        block = jnp.where(block < KEPT // 2, block, block + (ROWS - KEPT))
        index_y = block * BLOCK_Y + lax.bitwise_and(rows, 3) * 128 + lanes
        return jnp.where(index_y < LENGTH // 2, index_y, index_y - LENGTH)

    wave_y = wave_of((KEPT * 8, 128))
    kappa_y = wave_scale * wave_y.astype(FULL) / LENGTH
    keep_y = 3 * jnp.abs(wave_y) < LENGTH
    turn_cos = jnp.concatenate([line_turns[0], line_turns[0]], axis=1)
    turn_sin = jnp.concatenate([line_turns[1], line_turns[1]], axis=1)

    def line_in(l):
        await_bytes(got_one.at[l], line_sems.at[l])
        wave_x = l * BLOCK_X + own_line
        full_x = jnp.full((1, 128), wave_x, jnp.int32)
        kappa_x = wave_scale * full_x.astype(FULL) / LENGTH
        square = full_x * full_x + wave_y * wave_y
        inverse_sq = LENGTH * LENGTH / (9.0 * jnp.maximum(square, 1).astype(FULL))
        doubled = jnp.where(full_x == 0, 1.0, 2.0) * (1.0 / LENGTH)
        keep = keep_y & (3 * full_x < LENGTH)
        factor = jnp.where(keep, inverse_sq * doubled, 0.0)
        data = got_one[l]
        both = jnp.concatenate(
            [kappa_y * factor * data, -(kappa_x * factor) * data], axis=1
        )
        high, low = split(both)
        mixed = times(first_table[0], first_table[1], high, low)
        real, imag = mixed[:64], mixed[64:]
        out_real = real * turn_cos - imag * turn_sin
        out_imag = real * turn_sin + imag * turn_cos
        top, rest = split(jnp.concatenate([out_real, out_imag], axis=1))
        place = pl.ds(pl.multiple_of(l * 64, 64), 64)
        lines_high[place, :] = top
        lines_low[place, :] = rest

    def line_step(step, carry):
        l = col_at(step, -1)

        @pl.when(l < LINES)
        def _():
            line_in(l)

        return carry

    lax.fori_loop(0, COLS, line_step, 0)

    def post_column(source, destination, phase, peer_col, sem):
        def send(step, carry):
            peer_row = row_at(step)
            post(
                source.at[pl.ds((peer_col * ROWS + peer_row) * LINES, LINES)],
                destination.at[pl.ds(own * LINES, LINES)],
                phase,
                peer_row,
                peer_col,
                sem,
            )
            return carry

        lax.fori_loop(0, ROWS, send, 0)

    def quarter_out(step, carry):
        quarter = lax.rem(col // 4 + far_first(step), 4)
        high_part = jnp.dot(lines_high[...], second_table[quarter], preferred_element_type=FULL)
        low_part = jnp.dot(
            lines_low[...], second_table[quarter, :, 0:128], preferred_element_type=FULL
        )
        lines_full[:, 0:128] = (high_part[:, 128:256] + low_part) + high_part[:, 0:128]

        def place_line(l, inner):
            for group in range(8):
                sent_two[
                    pl.ds((quarter * 64 + group * 8) * LINES + l, 8, stride=LINES), :
                ] = lines_full[pl.ds(pl.multiple_of(l * 64, 64) + group * 8, 8), 0:128]
            return inner

        lax.fori_loop(0, LINES, place_line, 0)

        def send_quarter(offset, inner):
            peer_col = quarter * 4 + lax.rem(col + far_first(offset), 4)
            post_column(sent_two, got_two, 1, peer_col, column_sems.at[col])
            return inner

        lax.fori_loop(0, 4, send_quarter, 0)
        return carry

    lax.fori_loop(0, 4, quarter_out, 0)

    def linear(group, carry):
        place = pl.ds(pl.multiple_of(group * 8, 8), 8)
        shape = (8, BLOCK_Y)
        wave_x = col * BLOCK_X + group * 8 + lax.broadcasted_iota(jnp.int32, shape, 0)
        index_y = row * BLOCK_Y + lax.broadcasted_iota(jnp.int32, shape, 1)
        signed_y = jnp.where(index_y < LENGTH // 2, index_y, index_y - LENGTH)
        damping, weight_a, weight_b, weight_c = section_weights(wave_x, signed_y)
        weight_last[place, :] = weight_c
        for part in range(2):
            target[part, place, :] = (
                damping * start_field[part, place, :]
                + weight_a * start_term[part, place, :]
                + 2.0 * weight_b * (first_term[part, place, :] + second_term[part, place, :])
            )
        return carry

    lax.fori_loop(0, BLOCK_X // 8, linear, 0)
    turn_tables(1)

    lane = lax.broadcasted_iota(jnp.int32, (8, 128), 1)
    upper = lane >= 64

    def columns_in(step_in, carry):
        group = col_at(step_in, -1)
        await_bytes(
            got_two.at[pl.ds(group * ROWS * LINES, ROWS * LINES)], column_sems.at[group]
        )
        spread = []
        for high_bit in range(2):
            start = (high_bit * 8 + group * 16) * LINES
            spread.append(
                spread_lines(
                    [got_two[pl.ds(start + l, 8, stride=LINES), :] for l in range(LINES)],
                    upper,
                )
            )
        column = [None] * 64
        for step in range(32):
            other = spread[1][step]
            moved = total(
                [
                    scaled(cosine_of(step, 64), other),
                    scaled(sine_of(step, 64), turned(other, upper)) if step else None,
                ]
            )
            column[step] = spread[0][step] + moved
            column[step + 32] = spread[0][step] - moved
        place = pl.multiple_of(group * 8, 8)
        for step in range(PAIRS):
            value = column[step]
            if step % 32 == 0:
                real_part = jnp.where(upper, 0.0, value)
                imag_part = jnp.where(upper, 0.0, pltpu.roll(value, 64, 1))
            else:
                mirror = column[64 - step]
                real_part = jnp.where(upper, pltpu.roll(mirror, 64, 1), value)
                imag_part = jnp.where(upper, -mirror, pltpu.roll(value, 64, 1))
            points[step, pl.ds(place, 8), :] = real_part
            points[step, pl.ds(place + 128, 8), :] = imag_part
        return carry

    lax.fori_loop(0, 16, columns_in, 0)

    first_field = lax.broadcasted_iota(jnp.int32, (128, 128), 1) % 64 < 32

    def column_products(step, carry):
        for index in [11 * step + k for k in range(11)]:
            high, low = split(points[index])
            wide = jnp.dot(
                table[index],
                jnp.concatenate([high, low], axis=1),
                preferred_element_type=FULL,
            )
            grid = (wide[:128, 128:] + wide[128:, :128]) + wide[:128, :128]
            from_left = pltpu.roll(grid, 32, 1)
            from_right = pltpu.roll(grid, 96, 1)
            product = jnp.where(
                first_field, grid * from_right, (grid - from_left) * (grid + from_left)
            )
            both = jnp.concatenate(split(product), axis=1)
            wide = jnp.dot(
                back[index],
                jnp.concatenate([both, both], axis=0),
                preferred_element_type=FULL,
            )
            points[index] = wide[:, 128:] + wide[:, :128]
        return carry

    lax.fori_loop(0, PAIRS // 11, column_products, 0)

    def columns_out(step_out, carry):
        group = col_at(step_out, 1)
        place = pl.multiple_of(group * 8, 8)
        column = [None] * 64
        for step in range(PAIRS):
            real_part = points[step, pl.ds(place, 8), :]
            imag_part = points[step, pl.ds(place + 128, 8), :]
            column[step] = jnp.where(upper, pltpu.roll(imag_part, 64, 1), real_part)
            if step % 32:
                column[64 - step] = jnp.where(
                    upper, -imag_part, pltpu.roll(real_part, 64, 1)
                )
        sums, gaps = [], []
        for step in range(32):
            sums.append(column[step] + column[step + 32])
            gap = column[step] - column[step + 32]
            gaps.append(
                total(
                    [
                        scaled(cosine_of(step, 64), gap),
                        scaled(-sine_of(step, 64), turned(gap, upper)) if step else None,
                    ]
                )
            )
        for high_bit, values in enumerate((sums, gaps)):
            start = (high_bit * 8 + group * 16) * LINES
            for l, value in enumerate(gather_lines(values, upper)):
                sent_three[pl.ds(start + l, 8, stride=LINES), :] = value
        post_column(sent_three, got_three, 2, group, recv_sems.at[0])
        return carry

    lax.fori_loop(0, 16, columns_out, 0)

    await_bytes(got_three, recv_sems.at[0])

    def collect(l, carry):
        for quarter in range(4):
            for group in range(4):
                start = (quarter * 64 + group * 16) * LINES + l
                top, rest = split(
                    jnp.concatenate(
                        [
                            got_three[pl.ds(start, 8, stride=LINES), :],
                            got_three[pl.ds(start + 8 * LINES, 8, stride=LINES), :],
                        ]
                    )
                )
                place = pl.ds(pl.multiple_of(l * 64, 64) + group * 16, 16)
                lanes = slice(quarter * 128, quarter * 128 + 128)
                lines_high[place, lanes] = top
                lines_low[place, lanes] = rest
        return carry

    lax.fori_loop(0, LINES, collect, 0)

    for part, full in enumerate((lines_full, lines_imag)):
        wide = slice(256 * part, 256 * part + 256)
        full[...] = times(
            lines_high[...], lines_low[...], third_table[0, :, wide], third_table[1, :, wide]
        )

    def line_out(l):
        place = pl.ds(pl.multiple_of(l * 64, 64), 64)
        real, imag = lines_full[place, :], lines_imag[place, :]
        out_real = real * turn_cos + imag * turn_sin
        out_imag = imag * turn_cos - real * turn_sin
        high, low = split(jnp.concatenate([out_real, out_imag], axis=0))
        value = times(last_table[0], last_table[1], high, low)
        full_x = jnp.full((1, 128), l * BLOCK_X + own_line, jnp.int32)
        kappa_x = wave_scale * full_x.astype(FULL) / LENGTH
        scale = jnp.where(keep_y & (3 * full_x < LENGTH), 1.0 / LENGTH, 0.0)
        weight_cross = (kappa_x * kappa_x - kappa_y * kappa_y) * scale
        weight_gap = kappa_x * kappa_y * scale
        sent_four[l] = weight_cross * value[:, :128] + weight_gap * value[:, 128:]

        def send_term(step, inner):
            block = lax.rem(kept_row + step, KEPT)
            post(
                sent_four.at[l, pl.ds(pl.multiple_of(block * 8, 8), 8)],
                got_four.at[pl.ds(pl.multiple_of(own_line * 8, 8), 8)],
                3,
                jnp.where(block < KEPT // 2, block, block + (ROWS - KEPT)),
                l,
                recv_sems.at[1],
            )
            return inner

        lax.fori_loop(0, KEPT, send_term, 0)

    def line_out_step(step, carry):
        l = col_at(step, 1)

        @pl.when(l < LINES)
        def _():
            line_out(l)

        return carry

    lax.fori_loop(0, COLS, line_out_step, 0)

    @pl.when(holds)
    def _():
        await_bytes(got_four, recv_sems.at[1])

        def finish(group, carry):
            place = pl.ds(pl.multiple_of(group * 8, 8), 8)
            for part in range(2):
                for quarter in range(4):
                    lanes = slice(quarter * 128, quarter * 128 + 128)
                    start = pl.multiple_of(group * 64, 64) + (part * 4 + quarter)
                    target[part, place, lanes] = (
                        target[part, place, lanes]
                        + weight_last[place, lanes] * got_four[pl.ds(start, 8, stride=8), :]
                    )
            return carry

        lax.fori_loop(0, BLOCK_X // 8, finish, 0)
        others = sent_one.at[pl.ds(0, (DEVICES - 1) * 8)]
        await_bytes(others, send_sems.at[0])
        await_bytes(sent_four.at[0, pl.ds(0, KEPT * 8 - 8)], send_sems.at[3])
        await_bytes(sent_four.at[pl.ds(0, LINES - 1)], send_sems.at[3])

    @pl.when(jnp.logical_not(holds))
    def _():
        await_bytes(sent_four, send_sems.at[3])

    for phase, sent in ((1, sent_two), (2, sent_three)):
        await_bytes(sent.at[pl.ds(0, (DEVICES - 1) * LINES)], send_sems.at[phase])


def per_device(start_field, section_field, start_term, first_term, second_term):
    shape = (2, BLOCK_X, BLOCK_Y)
    fields = [
        field.reshape(shape)
        for field in (start_field, section_field, start_term, first_term, second_term)
    ]
    constants = [jnp.asarray(table) for table in tables()]
    vmem = pl.BlockSpec(memory_space=pltpu.VMEM)
    result = pl.pallas_call(
        section_kernel,
        out_shape=jax.ShapeDtypeStruct(shape, FULL),
        in_specs=[vmem] * (len(fields) + len(constants)),
        out_specs=vmem,
        scratch_shapes=[
            pltpu.VMEM((BLOCK_X * 8, 128), FULL),
            pltpu.VMEM((LINES, KEPT * 8, 128), FULL),
            pltpu.VMEM((DEVICES * LINES, 128), FULL),
            pltpu.VMEM((DEVICES * LINES, 128), FULL),
            pltpu.VMEM((DEVICES * LINES, 128), FULL),
            pltpu.VMEM((DEVICES * LINES, 128), FULL),
            pltpu.VMEM((LINES, KEPT * 8, 128), FULL),
            pltpu.VMEM((BLOCK_X * 8, 128), FULL),
            pltpu.VMEM((LINES * 64, 512), HIGH),
            pltpu.VMEM((LINES * 64, 512), HIGH),
            pltpu.VMEM((LINES * 64, 256), FULL),
            pltpu.VMEM((LINES * 64, 256), FULL),
            pltpu.VMEM((PAIRS, 256, 128), FULL),
            pltpu.VMEM((PAIRS, 256, 256), HIGH),
            pltpu.VMEM((PAIRS, 256, 256), HIGH),
            pltpu.VMEM((BLOCK_X, BLOCK_Y), FULL),
            pltpu.SemaphoreType.DMA((4,)),
            pltpu.SemaphoreType.DMA((2,)),
            pltpu.SemaphoreType.DMA((LINES,)),
            pltpu.SemaphoreType.DMA((COLS,)),
        ],
        compiler_params=pltpu.CompilerParams(
            has_side_effects=True, vmem_limit_bytes=56 * 2**20
        ),
        name="section",
    )(*fields, *constants)
    return result.reshape((1,) + shape)


def solution(mesh):
    spec = P(None, None, "col", "row")
    return jax.shard_map(
        per_device,
        mesh=mesh,
        in_specs=(spec,) * 5,
        out_specs=spec,
        check_vma=False,
    )
```

```python
import functools
import math

import jax
import jax.numpy as jnp
import ml_dtypes
import numpy as np
from jax import lax
from jax.experimental import pallas as pl
from jax.experimental.pallas import tpu as pltpu
from jax.sharding import PartitionSpec as P

LENGTH = 8192
ROWS = 16
COLS = 16
DEVICES = ROWS * COLS
BLOCK_X = 256
BLOCK_Y = 512
LINES = 11
KEPT = 12
PAIRS = 33

viscous_rate = 1.5
wave_scale = 3.0
series_terms = 12

HIGH = jnp.bfloat16
FULL = jnp.float32


def section_weights(wave_x, wave_y):
    square = wave_x * wave_x + wave_y * wave_y
    kappa_x = wave_scale * wave_x.astype(FULL) / LENGTH
    kappa_y = wave_scale * wave_y.astype(FULL) / LENGTH
    kappa_sq = kappa_x * kappa_x + kappa_y * kappa_y
    zvalue = -viscous_rate * kappa_sq
    damping = jnp.exp(zvalue)
    near_zero = 27 * square < 2 * LENGTH * LENGTH

    def series(degree):
        running = jnp.full_like(zvalue, 1.0 / math.factorial(series_terms - 1 + degree))
        for term_index in range(series_terms - 2, -1, -1):
            running = running * zvalue + 1.0 / math.factorial(term_index + degree)
        return running

    clamped = jnp.where(near_zero, -1.0, zvalue)
    exp_clamped = jnp.exp(clamped)
    closed_one = (exp_clamped - 1.0) / clamped
    closed_two = (exp_clamped - 1.0 - clamped) / (clamped * clamped)
    closed_three = (exp_clamped - 1.0 - clamped - 0.5 * clamped * clamped) / (
        clamped * clamped * clamped
    )
    phi_one = jnp.where(near_zero, series(1), closed_one)
    phi_two = jnp.where(near_zero, series(2), closed_two)
    phi_three = jnp.where(near_zero, series(3), closed_three)
    weight_a = phi_one - 3.0 * phi_two + 4.0 * phi_three
    weight_b = phi_two - 2.0 * phi_three
    weight_c = 4.0 * phi_three - phi_two
    return damping, weight_a, weight_b, weight_c


def halves(table):
    table = np.asarray(table, np.float32)
    high = table.astype(ml_dtypes.bfloat16)
    low = (table - high.astype(np.float32)).astype(ml_dtypes.bfloat16)
    return np.stack([high, low])


@functools.lru_cache(None)
def tables():
    row = np.arange(KEPT * 8)
    kept_row = row // 8
    source_row = np.where(kept_row < KEPT // 2, kept_row, kept_row + ROWS - KEPT)
    part = row % 8 // 4
    index_a = 4 * source_row + row % 4
    index_c = np.arange(64)
    angle = 2 * np.pi / 64 * (index_c[:, None] * index_a[None, :] % 64)
    cosine, sine = np.cos(angle), np.sin(angle)
    real_rows = np.where(part == 0, -sine, -cosine)
    imag_rows = np.where(part == 0, cosine, -sine)
    first = np.concatenate([real_rows, imag_rows])
    real_out = np.where(part == 0, cosine, -sine)
    imag_out = np.where(part == 0, sine, cosine)
    last = np.concatenate([real_out, imag_out]).T
    index_b = np.arange(128)
    turn = 2 * np.pi / LENGTH * (index_c[:, None] * index_b[None, :])
    turns = np.stack([np.cos(turn), np.sin(turn)]).astype(np.float32)
    angle = 2 * np.pi / 128 * (index_b[:, None] * index_b[None, :] % 128)
    cosine, sine = np.cos(angle), np.sin(angle)
    second = np.zeros((2, 2, 128, 4, 2, 2, 32))
    for field in range(2):
        second[0, field, :, :, 0, field] = cosine.reshape(128, 4, 32)
        second[0, field, :, :, 1, field] = sine.reshape(128, 4, 32)
        second[1, field, :, :, 0, field] = -sine.reshape(128, 4, 32)
        second[1, field, :, :, 1, field] = cosine.reshape(128, 4, 32)
    second = second.reshape(512, 512)
    spin = 2 * np.pi / LENGTH * np.broadcast_to(index_b[None, :], (128, 128))
    base = np.stack(
        [cosine, -sine, np.cos(spin), -np.sin(spin), np.cos(spin.T), -np.sin(spin.T)]
    ).astype(np.float32)
    wide = np.stack(
        [np.concatenate(halves(second[:, 128 * g : 128 * g + 128]), axis=1) for g in range(4)]
    )
    return halves(first), wide, halves(second.T), halves(last), turns, base


def split(values):
    high = values.astype(HIGH)
    return high, (values - high.astype(FULL)).astype(HIGH)


def times(left_high, left_low, right_high, right_low):
    dot = functools.partial(jnp.dot, preferred_element_type=FULL)
    return (
        dot(left_high, right_low) + dot(left_low, right_high)
    ) + dot(left_high, right_high)


def turned(values, upper):
    moved = pltpu.roll(values, 64, 1)
    return jnp.where(upper, moved, -moved)


def cosine_of(step, period):
    return math.cos(2 * math.pi * (step % period) / period)


def sine_of(step, period):
    return math.sin(2 * math.pi * (step % period) / period)


def scaled(factor, value):
    if abs(factor) < 1e-12:
        return None
    if abs(factor - 1) < 1e-12:
        return value
    if abs(factor + 1) < 1e-12:
        return -value
    return factor * value


def total(values):
    values = [value for value in values if value is not None]
    if not values:
        return None
    return functools.reduce(lambda a, b: a + b, values)


def plus(a, b):
    return b if a is None else a if b is None else a + b


def minus(a, b):
    return a if b is None else -b if a is None else a - b


def spread_lines(lines, upper):
    turns = [turned(line, upper) for line in lines]
    out = [None] * 32
    for step in range(9):
        sums = []
        for parity in range(2):
            picked = range(parity, LINES, 2)
            sums.append(total(scaled(cosine_of(l * step, 32), lines[l]) for l in picked))
            sums.append(total(scaled(sine_of(l * step, 32), turns[l]) for l in picked))
        cos_even, sin_even, cos_odd, sin_odd = sums
        cos_sum, cos_gap = plus(cos_even, cos_odd), minus(cos_even, cos_odd)
        sin_sum, sin_gap = plus(sin_even, sin_odd), minus(sin_even, sin_odd)
        out[step] = plus(cos_sum, sin_sum)
        out[(16 + step) % 32] = plus(cos_gap, sin_gap)
        if step:
            out[32 - step] = minus(cos_sum, sin_sum)
            out[16 - step] = minus(cos_gap, sin_gap)
    return out


def gather_lines(points, upper):
    out = [None] * LINES
    for parity in range(2):
        sign = 1 - 2 * parity
        folded = [
            points[step] + points[step + 16] if sign > 0 else points[step] - points[step + 16]
            for step in range(16)
        ]
        even, odd = [folded[0]], [None]
        for step in range(1, 8):
            mirror = folded[16 - step]
            even.append(folded[step] + mirror if sign > 0 else folded[step] - mirror)
            odd.append(
                turned(folded[step] - mirror if sign > 0 else folded[step] + mirror, upper)
            )
        even.append(folded[8])
        odd.append(turned(folded[8], upper))
        for l in range(parity, LINES, 2):
            terms = [scaled(cosine_of(l * step, 32), even[step]) for step in range(9)]
            terms += [scaled(-sine_of(l * step, 32), odd[step]) for step in range(1, 9)]
            out[l] = total(terms)
    return out


def section_kernel(
    start_field,
    section_field,
    start_term,
    first_term,
    second_term,
    first_table,
    second_table,
    third_table,
    last_table,
    line_turns,
    base,
    target,
    sent_one,
    got_one,
    sent_two,
    got_two,
    sent_three,
    got_three,
    sent_four,
    got_four,
    lines_high,
    lines_low,
    lines_full,
    lines_imag,
    points,
    table,
    back,
    weight_last,
    send_sems,
    recv_sems,
    line_sems,
    column_sems,
):
    row, col = lax.axis_index("row"), lax.axis_index("col")
    own = col * ROWS + row
    own_line = col * 8 + lax.rem(row, 8) + 128 * (row // 8)
    lower_half = row < KEPT // 2
    holds = (col < LINES) & (lower_half | (row >= ROWS - KEPT // 2))
    kept_row = jnp.where(lower_half, row, jnp.where(row >= ROWS - KEPT // 2, row - 4, 0))
    kept_col = jnp.where(col < LINES, col, 0)

    def far_first(step):
        back_step = 3 - step
        return lax.bitwise_xor(back_step, lax.shift_right_logical(back_step, 1))

    def col_at(step, sign):
        across = lax.rem(col // 4 + 4 + sign * far_first(step // 4), 4)
        along = lax.rem(lax.rem(col, 4) + 4 + sign * far_first(lax.rem(step, 4)), 4)
        return 4 * across + along

    def col_far(step, sign):
        across = lax.rem(col // 4 + 4 + sign * far_first(lax.rem(step, 4)), 4)
        along = lax.rem(lax.rem(col, 4) + 4 + sign * far_first(step // 4), 4)
        return 4 * across + along

    def row_at(step):
        across = lax.rem(row // 4 + far_first(step // 4), 4)
        return 4 * across + lax.bitwise_xor(lax.rem(row, 4), 3 - lax.rem(step, 4))

    def post(source, destination, phase, peer_row, peer_col, sem):
        itself = (peer_row == row) & (peer_col == col)

        @pl.when(itself)
        def _():
            pltpu.make_async_copy(source, destination, sem).start()

        @pl.when(jnp.logical_not(itself))
        def _():
            pltpu.make_async_remote_copy(
                source,
                destination,
                send_sems.at[phase],
                sem,
                device_id={"row": peer_row, "col": peer_col},
                device_id_type=pl.DeviceIdType.MESH,
            ).start()

    def await_bytes(ref, sem):
        pltpu.make_async_copy(ref, ref, sem).wait()

    def shuffle(group, carry):
        for part in range(2):
            for quarter in range(4):
                start = pl.multiple_of(group * 64, 64) + (part * 4 + quarter)
                sent_one[pl.ds(start, 8, stride=8), :] = section_field[
                    part,
                    pl.ds(pl.multiple_of(group * 8, 8), 8),
                    quarter * 128 : quarter * 128 + 128,
                ]
        return carry

    @pl.when(holds)
    def _():
        lax.fori_loop(0, BLOCK_X // 8, shuffle, 0)

        def send(step, carry):
            peer_row = row_at(lax.rem(step, ROWS))
            peer_col = col_far(step // ROWS, 1)
            line = peer_col * 8 + lax.rem(peer_row, 8) + 128 * (peer_row // 8)
            post(
                sent_one.at[pl.ds(pl.multiple_of(line * 8, 8), 8)],
                got_one.at[kept_col, pl.ds(pl.multiple_of(kept_row * 8, 8), 8)],
                0,
                peer_row,
                peer_col,
                line_sems.at[kept_col],
            )
            return carry

        lax.fori_loop(0, DEVICES, send, 0)

    def turn_tables(flip):
        def step(index, carry):
            cosine, sine = carry
            for place, value in enumerate((cosine, sine)):
                top, rest = split(value)
                span = slice(128 * place, 128 * place + 128)
                if flip:
                    back[index, span, 0:128] = top
                    back[index, span, 128:256] = rest
                else:
                    table[index, 0:128, span] = top
                    table[index, 128:256, span] = rest
            spin_cos, spin_sin = base[2 + 2 * flip], base[3 + 2 * flip]
            return (
                cosine * spin_cos - sine * spin_sin,
                cosine * spin_sin + sine * spin_cos,
            )

        lax.fori_loop(0, PAIRS, step, (base[0], base[1]))

    turn_tables(0)

    def wave_of(rows_shape):
        rows = lax.broadcasted_iota(jnp.int32, rows_shape, 0)
        lanes = lax.broadcasted_iota(jnp.int32, rows_shape, 1)
        block = lax.shift_right_logical(rows, 3)
        block = jnp.where(block < KEPT // 2, block, block + (ROWS - KEPT))
        index_y = block * BLOCK_Y + lax.bitwise_and(rows, 3) * 128 + lanes
        return jnp.where(index_y < LENGTH // 2, index_y, index_y - LENGTH)

    wave_y = wave_of((KEPT * 8, 128))
    kappa_y = wave_scale * wave_y.astype(FULL) / LENGTH
    keep_y = 3 * jnp.abs(wave_y) < LENGTH
    turn_cos = jnp.concatenate([line_turns[0], line_turns[0]], axis=1)
    turn_sin = jnp.concatenate([line_turns[1], line_turns[1]], axis=1)

    def line_in(l):
        await_bytes(got_one.at[l], line_sems.at[l])
        wave_x = l * BLOCK_X + own_line
        full_x = jnp.full((1, 128), wave_x, jnp.int32)
        kappa_x = wave_scale * full_x.astype(FULL) / LENGTH
        square = full_x * full_x + wave_y * wave_y
        inverse_sq = LENGTH * LENGTH / (9.0 * jnp.maximum(square, 1).astype(FULL))
        doubled = jnp.where(full_x == 0, 1.0, 2.0) * (1.0 / LENGTH)
        keep = keep_y & (3 * full_x < LENGTH)
        factor = jnp.where(keep, inverse_sq * doubled, 0.0)
        data = got_one[l]
        both = jnp.concatenate(
            [kappa_y * factor * data, -(kappa_x * factor) * data], axis=1
        )
        high, low = split(both)
        mixed = times(first_table[0], first_table[1], high, low)
        real, imag = mixed[:64], mixed[64:]
        out_real = real * turn_cos - imag * turn_sin
        out_imag = real * turn_sin + imag * turn_cos
        top, rest = split(jnp.concatenate([out_real, out_imag], axis=1))
        place = pl.ds(pl.multiple_of(l * 64, 64), 64)
        lines_high[place, :] = top
        lines_low[place, :] = rest

    def line_step(step, carry):
        l = col_far(step, -1)

        @pl.when(l < LINES)
        def _():
            line_in(l)

        return carry

    lax.fori_loop(0, COLS, line_step, 0)

    def post_column(source, destination, phase, peer_col, sem):
        def send(step, carry):
            peer_row = row_at(step)
            post(
                source.at[pl.ds((peer_col * ROWS + peer_row) * LINES, LINES)],
                destination.at[pl.ds(own * LINES, LINES)],
                phase,
                peer_row,
                peer_col,
                sem,
            )
            return carry

        lax.fori_loop(0, ROWS, send, 0)

    def quarter_out(step, carry):
        quarter = lax.rem(col // 4 + far_first(step), 4)
        high_part = jnp.dot(lines_high[...], second_table[quarter], preferred_element_type=FULL)
        low_part = jnp.dot(
            lines_low[...], second_table[quarter, :, 0:128], preferred_element_type=FULL
        )
        lines_full[:, 0:128] = (high_part[:, 128:256] + low_part) + high_part[:, 0:128]

        def place_line(l, inner):
            for group in range(8):
                sent_two[
                    pl.ds((quarter * 64 + group * 8) * LINES + l, 8, stride=LINES), :
                ] = lines_full[pl.ds(pl.multiple_of(l * 64, 64) + group * 8, 8), 0:128]
            return inner

        lax.fori_loop(0, LINES, place_line, 0)

        def send_quarter(offset, inner):
            peer_col = quarter * 4 + lax.rem(col + far_first(offset), 4)
            post_column(sent_two, got_two, 1, peer_col, column_sems.at[col])
            return inner

        lax.fori_loop(0, 4, send_quarter, 0)
        return carry

    lax.fori_loop(0, 4, quarter_out, 0)

    def linear(group, carry):
        place = pl.ds(pl.multiple_of(group * 8, 8), 8)
        shape = (8, BLOCK_Y)
        wave_x = col * BLOCK_X + group * 8 + lax.broadcasted_iota(jnp.int32, shape, 0)
        index_y = row * BLOCK_Y + lax.broadcasted_iota(jnp.int32, shape, 1)
        signed_y = jnp.where(index_y < LENGTH // 2, index_y, index_y - LENGTH)
        damping, weight_a, weight_b, weight_c = section_weights(wave_x, signed_y)
        weight_last[place, :] = weight_c
        for part in range(2):
            target[part, place, :] = (
                damping * start_field[part, place, :]
                + weight_a * start_term[part, place, :]
                + 2.0 * weight_b * (first_term[part, place, :] + second_term[part, place, :])
            )
        return carry

    lax.fori_loop(0, BLOCK_X // 8, linear, 0)
    turn_tables(1)

    lane = lax.broadcasted_iota(jnp.int32, (8, 128), 1)
    upper = lane >= 64

    def columns_in(step_in, carry):
        group = col_at(step_in, -1)
        await_bytes(
            got_two.at[pl.ds(group * ROWS * LINES, ROWS * LINES)], column_sems.at[group]
        )
        spread = []
        for high_bit in range(2):
            start = (high_bit * 8 + group * 16) * LINES
            spread.append(
                spread_lines(
                    [got_two[pl.ds(start + l, 8, stride=LINES), :] for l in range(LINES)],
                    upper,
                )
            )
        column = [None] * 64
        for step in range(32):
            other = spread[1][step]
            moved = total(
                [
                    scaled(cosine_of(step, 64), other),
                    scaled(sine_of(step, 64), turned(other, upper)) if step else None,
                ]
            )
            column[step] = spread[0][step] + moved
            column[step + 32] = spread[0][step] - moved
        place = pl.multiple_of(group * 8, 8)
        for step in range(PAIRS):
            value = column[step]
            if step % 32 == 0:
                real_part = jnp.where(upper, 0.0, value)
                imag_part = jnp.where(upper, 0.0, pltpu.roll(value, 64, 1))
            else:
                mirror = column[64 - step]
                real_part = jnp.where(upper, pltpu.roll(mirror, 64, 1), value)
                imag_part = jnp.where(upper, -mirror, pltpu.roll(value, 64, 1))
            points[step, pl.ds(place, 8), :] = real_part
            points[step, pl.ds(place + 128, 8), :] = imag_part
        return carry

    lax.fori_loop(0, 16, columns_in, 0)

    first_field = lax.broadcasted_iota(jnp.int32, (128, 128), 1) % 64 < 32

    def column_products(step, carry):
        for index in [11 * step + k for k in range(11)]:
            high, low = split(points[index])
            wide = jnp.dot(
                table[index],
                jnp.concatenate([high, low], axis=1),
                preferred_element_type=FULL,
            )
            grid = (wide[:128, 128:] + wide[128:, :128]) + wide[:128, :128]
            from_left = pltpu.roll(grid, 32, 1)
            from_right = pltpu.roll(grid, 96, 1)
            product = jnp.where(
                first_field, grid * from_right, (grid - from_left) * (grid + from_left)
            )
            both = jnp.concatenate(split(product), axis=1)
            wide = jnp.dot(
                back[index],
                jnp.concatenate([both, both], axis=0),
                preferred_element_type=FULL,
            )
            points[index] = wide[:, 128:] + wide[:, :128]
        return carry

    lax.fori_loop(0, PAIRS // 11, column_products, 0)

    def columns_out(step_out, carry):
        group = col_far(step_out, 1)
        place = pl.multiple_of(group * 8, 8)
        column = [None] * 64
        for step in range(PAIRS):
            real_part = points[step, pl.ds(place, 8), :]
            imag_part = points[step, pl.ds(place + 128, 8), :]
            column[step] = jnp.where(upper, pltpu.roll(imag_part, 64, 1), real_part)
            if step % 32:
                column[64 - step] = jnp.where(
                    upper, -imag_part, pltpu.roll(real_part, 64, 1)
                )
        sums, gaps = [], []
        for step in range(32):
            sums.append(column[step] + column[step + 32])
            gap = column[step] - column[step + 32]
            gaps.append(
                total(
                    [
                        scaled(cosine_of(step, 64), gap),
                        scaled(-sine_of(step, 64), turned(gap, upper)) if step else None,
                    ]
                )
            )
        for high_bit, values in enumerate((sums, gaps)):
            start = (high_bit * 8 + group * 16) * LINES
            for l, value in enumerate(gather_lines(values, upper)):
                sent_three[pl.ds(start + l, 8, stride=LINES), :] = value
        post_column(sent_three, got_three, 2, group, recv_sems.at[0])
        return carry

    lax.fori_loop(0, 16, columns_out, 0)

    await_bytes(got_three, recv_sems.at[0])

    def collect(l, carry):
        for quarter in range(4):
            for group in range(4):
                start = (quarter * 64 + group * 16) * LINES + l
                top, rest = split(
                    jnp.concatenate(
                        [
                            got_three[pl.ds(start, 8, stride=LINES), :],
                            got_three[pl.ds(start + 8 * LINES, 8, stride=LINES), :],
                        ]
                    )
                )
                place = pl.ds(pl.multiple_of(l * 64, 64) + group * 16, 16)
                lanes = slice(quarter * 128, quarter * 128 + 128)
                lines_high[place, lanes] = top
                lines_low[place, lanes] = rest
        return carry

    lax.fori_loop(0, LINES, collect, 0)

    for part, full in enumerate((lines_full, lines_imag)):
        wide = slice(256 * part, 256 * part + 256)
        full[...] = times(
            lines_high[...], lines_low[...], third_table[0, :, wide], third_table[1, :, wide]
        )

    def line_out(l):
        place = pl.ds(pl.multiple_of(l * 64, 64), 64)
        real, imag = lines_full[place, :], lines_imag[place, :]
        out_real = real * turn_cos + imag * turn_sin
        out_imag = imag * turn_cos - real * turn_sin
        high, low = split(jnp.concatenate([out_real, out_imag], axis=0))
        value = times(last_table[0], last_table[1], high, low)
        full_x = jnp.full((1, 128), l * BLOCK_X + own_line, jnp.int32)
        kappa_x = wave_scale * full_x.astype(FULL) / LENGTH
        scale = jnp.where(keep_y & (3 * full_x < LENGTH), 1.0 / LENGTH, 0.0)
        weight_cross = (kappa_x * kappa_x - kappa_y * kappa_y) * scale
        weight_gap = kappa_x * kappa_y * scale
        sent_four[l] = weight_cross * value[:, :128] + weight_gap * value[:, 128:]

        def send_term(step, inner):
            block = lax.rem(kept_row + step, KEPT)
            post(
                sent_four.at[l, pl.ds(pl.multiple_of(block * 8, 8), 8)],
                got_four.at[pl.ds(pl.multiple_of(own_line * 8, 8), 8)],
                3,
                jnp.where(block < KEPT // 2, block, block + (ROWS - KEPT)),
                l,
                recv_sems.at[1],
            )
            return inner

        lax.fori_loop(0, KEPT, send_term, 0)

    def line_out_step(step, carry):
        l = col_far(step, 1)

        @pl.when(l < LINES)
        def _():
            line_out(l)

        return carry

    lax.fori_loop(0, COLS, line_out_step, 0)

    @pl.when(holds)
    def _():
        await_bytes(got_four, recv_sems.at[1])

        def finish(group, carry):
            place = pl.ds(pl.multiple_of(group * 8, 8), 8)
            for part in range(2):
                for quarter in range(4):
                    lanes = slice(quarter * 128, quarter * 128 + 128)
                    start = pl.multiple_of(group * 64, 64) + (part * 4 + quarter)
                    target[part, place, lanes] = (
                        target[part, place, lanes]
                        + weight_last[place, lanes] * got_four[pl.ds(start, 8, stride=8), :]
                    )
            return carry

        lax.fori_loop(0, BLOCK_X // 8, finish, 0)
        others = sent_one.at[pl.ds(0, (DEVICES - 1) * 8)]
        await_bytes(others, send_sems.at[0])
        await_bytes(sent_four.at[0, pl.ds(0, KEPT * 8 - 8)], send_sems.at[3])
        await_bytes(sent_four.at[pl.ds(0, LINES - 1)], send_sems.at[3])

    @pl.when(jnp.logical_not(holds))
    def _():
        await_bytes(sent_four, send_sems.at[3])

    for phase, sent in ((1, sent_two), (2, sent_three)):
        await_bytes(sent.at[pl.ds(0, (DEVICES - 1) * LINES)], send_sems.at[phase])


def per_device(start_field, section_field, start_term, first_term, second_term):
    shape = (2, BLOCK_X, BLOCK_Y)
    fields = [
        field.reshape(shape)
        for field in (start_field, section_field, start_term, first_term, second_term)
    ]
    constants = [jnp.asarray(table) for table in tables()]
    vmem = pl.BlockSpec(memory_space=pltpu.VMEM)
    result = pl.pallas_call(
        section_kernel,
        out_shape=jax.ShapeDtypeStruct(shape, FULL),
        in_specs=[vmem] * (len(fields) + len(constants)),
        out_specs=vmem,
        scratch_shapes=[
            pltpu.VMEM((BLOCK_X * 8, 128), FULL),
            pltpu.VMEM((LINES, KEPT * 8, 128), FULL),
            pltpu.VMEM((DEVICES * LINES, 128), FULL),
            pltpu.VMEM((DEVICES * LINES, 128), FULL),
            pltpu.VMEM((DEVICES * LINES, 128), FULL),
            pltpu.VMEM((DEVICES * LINES, 128), FULL),
            pltpu.VMEM((LINES, KEPT * 8, 128), FULL),
            pltpu.VMEM((BLOCK_X * 8, 128), FULL),
            pltpu.VMEM((LINES * 64, 512), HIGH),
            pltpu.VMEM((LINES * 64, 512), HIGH),
            pltpu.VMEM((LINES * 64, 256), FULL),
            pltpu.VMEM((LINES * 64, 256), FULL),
            pltpu.VMEM((PAIRS, 256, 128), FULL),
            pltpu.VMEM((PAIRS, 256, 256), HIGH),
            pltpu.VMEM((PAIRS, 256, 256), HIGH),
            pltpu.VMEM((BLOCK_X, BLOCK_Y), FULL),
            pltpu.SemaphoreType.DMA((4,)),
            pltpu.SemaphoreType.DMA((2,)),
            pltpu.SemaphoreType.DMA((LINES,)),
            pltpu.SemaphoreType.DMA((COLS,)),
        ],
        compiler_params=pltpu.CompilerParams(
            has_side_effects=True, vmem_limit_bytes=56 * 2**20
        ),
        name="section",
    )(*fields, *constants)
    return result.reshape((1,) + shape)


def solution(mesh):
    spec = P(None, None, "col", "row")
    return jax.shard_map(
        per_device,
        mesh=mesh,
        in_specs=(spec,) * 5,
        out_specs=spec,
        check_vma=False,
    )
```

```python
import functools
import math

import jax
import jax.numpy as jnp
import ml_dtypes
import numpy as np
from jax import lax
from jax.experimental import pallas as pl
from jax.experimental.pallas import tpu as pltpu
from jax.sharding import PartitionSpec as P

LENGTH = 8192
ROWS = 16
COLS = 16
DEVICES = ROWS * COLS
BLOCK_X = 256
BLOCK_Y = 512
LINES = 11
KEPT = 12
PAIRS = 33

viscous_rate = 1.5
wave_scale = 3.0
series_terms = 12

HIGH = jnp.bfloat16
FULL = jnp.float32


def section_weights(wave_x, wave_y):
    square = wave_x * wave_x + wave_y * wave_y
    kappa_x = wave_scale * wave_x.astype(FULL) / LENGTH
    kappa_y = wave_scale * wave_y.astype(FULL) / LENGTH
    kappa_sq = kappa_x * kappa_x + kappa_y * kappa_y
    zvalue = -viscous_rate * kappa_sq
    damping = jnp.exp(zvalue)
    near_zero = 27 * square < 2 * LENGTH * LENGTH

    def series(degree):
        running = jnp.full_like(zvalue, 1.0 / math.factorial(series_terms - 1 + degree))
        for term_index in range(series_terms - 2, -1, -1):
            running = running * zvalue + 1.0 / math.factorial(term_index + degree)
        return running

    clamped = jnp.where(near_zero, -1.0, zvalue)
    exp_clamped = jnp.exp(clamped)
    closed_one = (exp_clamped - 1.0) / clamped
    closed_two = (exp_clamped - 1.0 - clamped) / (clamped * clamped)
    closed_three = (exp_clamped - 1.0 - clamped - 0.5 * clamped * clamped) / (
        clamped * clamped * clamped
    )
    phi_one = jnp.where(near_zero, series(1), closed_one)
    phi_two = jnp.where(near_zero, series(2), closed_two)
    phi_three = jnp.where(near_zero, series(3), closed_three)
    weight_a = phi_one - 3.0 * phi_two + 4.0 * phi_three
    weight_b = phi_two - 2.0 * phi_three
    weight_c = 4.0 * phi_three - phi_two
    return damping, weight_a, weight_b, weight_c


def halves(table):
    table = np.asarray(table, np.float32)
    high = table.astype(ml_dtypes.bfloat16)
    low = (table - high.astype(np.float32)).astype(ml_dtypes.bfloat16)
    return np.stack([high, low])


@functools.lru_cache(None)
def tables():
    row = np.arange(KEPT * 8)
    kept_row = row // 8
    source_row = np.where(kept_row < KEPT // 2, kept_row, kept_row + ROWS - KEPT)
    part = row % 8 // 4
    index_a = 4 * source_row + row % 4
    index_c = np.arange(64)
    angle = 2 * np.pi / 64 * (index_c[:, None] * index_a[None, :] % 64)
    cosine, sine = np.cos(angle), np.sin(angle)
    real_rows = np.where(part == 0, -sine, -cosine)
    imag_rows = np.where(part == 0, cosine, -sine)
    first = np.concatenate([real_rows, imag_rows])
    real_out = np.where(part == 0, cosine, -sine)
    imag_out = np.where(part == 0, sine, cosine)
    last = np.concatenate([real_out, imag_out]).T
    index_b = np.arange(128)
    turn = 2 * np.pi / LENGTH * (index_c[:, None] * index_b[None, :])
    turns = np.stack([np.cos(turn), np.sin(turn)]).astype(np.float32)
    angle = 2 * np.pi / 128 * (index_b[:, None] * index_b[None, :] % 128)
    cosine, sine = np.cos(angle), np.sin(angle)
    second = np.zeros((2, 2, 128, 4, 2, 2, 32))
    for field in range(2):
        second[0, field, :, :, 0, field] = cosine.reshape(128, 4, 32)
        second[0, field, :, :, 1, field] = sine.reshape(128, 4, 32)
        second[1, field, :, :, 0, field] = -sine.reshape(128, 4, 32)
        second[1, field, :, :, 1, field] = cosine.reshape(128, 4, 32)
    second = second.reshape(512, 512)
    spin = 2 * np.pi / LENGTH * np.broadcast_to(index_b[None, :], (128, 128))
    base = np.stack(
        [cosine, -sine, np.cos(spin), -np.sin(spin), np.cos(spin.T), -np.sin(spin.T)]
    ).astype(np.float32)
    wide = np.stack(
        [np.concatenate(halves(second[:, 128 * g : 128 * g + 128]), axis=1) for g in range(4)]
    )
    return halves(first), wide, halves(second.T), halves(last), turns, base


def split(values):
    high = values.astype(HIGH)
    return high, (values - high.astype(FULL)).astype(HIGH)


def times(left_high, left_low, right_high, right_low):
    dot = functools.partial(jnp.dot, preferred_element_type=FULL)
    return (
        dot(left_high, right_low) + dot(left_low, right_high)
    ) + dot(left_high, right_high)


def turned(values, upper):
    moved = pltpu.roll(values, 64, 1)
    return jnp.where(upper, moved, -moved)


def cosine_of(step, period):
    return math.cos(2 * math.pi * (step % period) / period)


def sine_of(step, period):
    return math.sin(2 * math.pi * (step % period) / period)


def scaled(factor, value):
    if abs(factor) < 1e-12:
        return None
    if abs(factor - 1) < 1e-12:
        return value
    if abs(factor + 1) < 1e-12:
        return -value
    return factor * value


def total(values):
    values = [value for value in values if value is not None]
    if not values:
        return None
    return functools.reduce(lambda a, b: a + b, values)


def plus(a, b):
    return b if a is None else a if b is None else a + b


def minus(a, b):
    return a if b is None else -b if a is None else a - b


def spread_lines(lines, upper):
    turns = [turned(line, upper) for line in lines]
    out = [None] * 32
    for step in range(9):
        sums = []
        for parity in range(2):
            picked = range(parity, LINES, 2)
            sums.append(total(scaled(cosine_of(l * step, 32), lines[l]) for l in picked))
            sums.append(total(scaled(sine_of(l * step, 32), turns[l]) for l in picked))
        cos_even, sin_even, cos_odd, sin_odd = sums
        cos_sum, cos_gap = plus(cos_even, cos_odd), minus(cos_even, cos_odd)
        sin_sum, sin_gap = plus(sin_even, sin_odd), minus(sin_even, sin_odd)
        out[step] = plus(cos_sum, sin_sum)
        out[(16 + step) % 32] = plus(cos_gap, sin_gap)
        if step:
            out[32 - step] = minus(cos_sum, sin_sum)
            out[16 - step] = minus(cos_gap, sin_gap)
    return out


def gather_lines(points, upper):
    out = [None] * LINES
    for parity in range(2):
        sign = 1 - 2 * parity
        folded = [
            points[step] + points[step + 16] if sign > 0 else points[step] - points[step + 16]
            for step in range(16)
        ]
        even, odd = [folded[0]], [None]
        for step in range(1, 8):
            mirror = folded[16 - step]
            even.append(folded[step] + mirror if sign > 0 else folded[step] - mirror)
            odd.append(
                turned(folded[step] - mirror if sign > 0 else folded[step] + mirror, upper)
            )
        even.append(folded[8])
        odd.append(turned(folded[8], upper))
        for l in range(parity, LINES, 2):
            terms = [scaled(cosine_of(l * step, 32), even[step]) for step in range(9)]
            terms += [scaled(-sine_of(l * step, 32), odd[step]) for step in range(1, 9)]
            out[l] = total(terms)
    return out


def section_kernel(
    start_field,
    section_field,
    start_term,
    first_term,
    second_term,
    first_table,
    second_table,
    third_table,
    last_table,
    line_turns,
    base,
    target,
    sent_one,
    got_one,
    sent_two,
    got_two,
    sent_three,
    got_three,
    sent_four,
    got_four,
    lines_high,
    lines_low,
    lines_full,
    lines_imag,
    points,
    table,
    back,
    weight_last,
    send_sems,
    recv_sems,
    line_sems,
    column_sems,
):
    row, col = lax.axis_index("row"), lax.axis_index("col")
    own = col * ROWS + row
    own_line = col * 8 + lax.rem(row, 8) + 128 * (row // 8)
    lower_half = row < KEPT // 2
    holds = (col < LINES) & (lower_half | (row >= ROWS - KEPT // 2))
    kept_row = jnp.where(lower_half, row, jnp.where(row >= ROWS - KEPT // 2, row - 4, 0))
    kept_col = jnp.where(col < LINES, col, 0)

    def far_first(step):
        back_step = 3 - step
        return lax.bitwise_xor(back_step, lax.shift_right_logical(back_step, 1))

    def col_at(step, sign):
        across = lax.rem(col // 4 + 4 + sign * far_first(step // 4), 4)
        along = lax.rem(lax.rem(col, 4) + 4 + sign * far_first(lax.rem(step, 4)), 4)
        return 4 * across + along

    def col_far(step, sign):
        across = lax.rem(col // 4 + 4 + sign * far_first(lax.rem(step, 4)), 4)
        along = lax.rem(lax.rem(col, 4) + 4 + sign * far_first(step // 4), 4)
        return 4 * across + along

    def row_at(step):
        across = lax.rem(row // 4 + far_first(step // 4), 4)
        return 4 * across + lax.bitwise_xor(lax.rem(row, 4), 3 - lax.rem(step, 4))

    def post(source, destination, phase, peer_row, peer_col, sem):
        itself = (peer_row == row) & (peer_col == col)

        @pl.when(itself)
        def _():
            pltpu.make_async_copy(source, destination, sem).start()

        @pl.when(jnp.logical_not(itself))
        def _():
            pltpu.make_async_remote_copy(
                source,
                destination,
                send_sems.at[phase],
                sem,
                device_id={"row": peer_row, "col": peer_col},
                device_id_type=pl.DeviceIdType.MESH,
            ).start()

    def await_bytes(ref, sem):
        pltpu.make_async_copy(ref, ref, sem).wait()

    def shuffle(group, carry):
        for part in range(2):
            for quarter in range(4):
                start = pl.multiple_of(group * 64, 64) + (part * 4 + quarter)
                sent_one[pl.ds(start, 8, stride=8), :] = section_field[
                    part,
                    pl.ds(pl.multiple_of(group * 8, 8), 8),
                    quarter * 128 : quarter * 128 + 128,
                ]
        return carry

    @pl.when(holds)
    def _():
        lax.fori_loop(0, BLOCK_X // 8, shuffle, 0)

        def send(step, carry):
            peer_row = row_at(step // COLS)
            peer_col = col_far(lax.rem(step, COLS), 1)
            line = peer_col * 8 + lax.rem(peer_row, 8) + 128 * (peer_row // 8)
            post(
                sent_one.at[pl.ds(pl.multiple_of(line * 8, 8), 8)],
                got_one.at[kept_col, pl.ds(pl.multiple_of(kept_row * 8, 8), 8)],
                0,
                peer_row,
                peer_col,
                line_sems.at[kept_col],
            )
            return carry

        lax.fori_loop(0, DEVICES, send, 0)

    def turn_tables(flip):
        def step(index, carry):
            cosine, sine = carry
            for place, value in enumerate((cosine, sine)):
                top, rest = split(value)
                span = slice(128 * place, 128 * place + 128)
                if flip:
                    back[index, span, 0:128] = top
                    back[index, span, 128:256] = rest
                else:
                    table[index, 0:128, span] = top
                    table[index, 128:256, span] = rest
            spin_cos, spin_sin = base[2 + 2 * flip], base[3 + 2 * flip]
            return (
                cosine * spin_cos - sine * spin_sin,
                cosine * spin_sin + sine * spin_cos,
            )

        lax.fori_loop(0, PAIRS, step, (base[0], base[1]))

    turn_tables(0)

    def wave_of(rows_shape):
        rows = lax.broadcasted_iota(jnp.int32, rows_shape, 0)
        lanes = lax.broadcasted_iota(jnp.int32, rows_shape, 1)
        block = lax.shift_right_logical(rows, 3)
        block = jnp.where(block < KEPT // 2, block, block + (ROWS - KEPT))
        index_y = block * BLOCK_Y + lax.bitwise_and(rows, 3) * 128 + lanes
        return jnp.where(index_y < LENGTH // 2, index_y, index_y - LENGTH)

    wave_y = wave_of((KEPT * 8, 128))
    kappa_y = wave_scale * wave_y.astype(FULL) / LENGTH
    keep_y = 3 * jnp.abs(wave_y) < LENGTH
    turn_cos = jnp.concatenate([line_turns[0], line_turns[0]], axis=1)
    turn_sin = jnp.concatenate([line_turns[1], line_turns[1]], axis=1)

    def line_in(l):
        await_bytes(got_one.at[l], line_sems.at[l])
        wave_x = l * BLOCK_X + own_line
        full_x = jnp.full((1, 128), wave_x, jnp.int32)
        kappa_x = wave_scale * full_x.astype(FULL) / LENGTH
        square = full_x * full_x + wave_y * wave_y
        inverse_sq = LENGTH * LENGTH / (9.0 * jnp.maximum(square, 1).astype(FULL))
        doubled = jnp.where(full_x == 0, 1.0, 2.0) * (1.0 / LENGTH)
        keep = keep_y & (3 * full_x < LENGTH)
        factor = jnp.where(keep, inverse_sq * doubled, 0.0)
        data = got_one[l]
        both = jnp.concatenate(
            [kappa_y * factor * data, -(kappa_x * factor) * data], axis=1
        )
        high, low = split(both)
        mixed = times(first_table[0], first_table[1], high, low)
        real, imag = mixed[:64], mixed[64:]
        out_real = real * turn_cos - imag * turn_sin
        out_imag = real * turn_sin + imag * turn_cos
        top, rest = split(jnp.concatenate([out_real, out_imag], axis=1))
        place = pl.ds(pl.multiple_of(l * 64, 64), 64)
        lines_high[place, :] = top
        lines_low[place, :] = rest

    def line_step(step, carry):
        l = col_at(step, -1)

        @pl.when(l < LINES)
        def _():
            line_in(l)

        return carry

    lax.fori_loop(0, COLS, line_step, 0)

    def post_column(source, destination, phase, peer_col, sem):
        def send(step, carry):
            peer_row = row_at(step)
            post(
                source.at[pl.ds((peer_col * ROWS + peer_row) * LINES, LINES)],
                destination.at[pl.ds(own * LINES, LINES)],
                phase,
                peer_row,
                peer_col,
                sem,
            )
            return carry

        lax.fori_loop(0, ROWS, send, 0)

    def quarter_out(step, carry):
        quarter = lax.rem(col // 4 + far_first(step), 4)
        high_part = jnp.dot(lines_high[...], second_table[quarter], preferred_element_type=FULL)
        low_part = jnp.dot(
            lines_low[...], second_table[quarter, :, 0:128], preferred_element_type=FULL
        )
        lines_full[:, 0:128] = (high_part[:, 128:256] + low_part) + high_part[:, 0:128]

        def place_line(l, inner):
            for group in range(8):
                sent_two[
                    pl.ds((quarter * 64 + group * 8) * LINES + l, 8, stride=LINES), :
                ] = lines_full[pl.ds(pl.multiple_of(l * 64, 64) + group * 8, 8), 0:128]
            return inner

        lax.fori_loop(0, LINES, place_line, 0)

        def send_quarter(offset, inner):
            peer_col = quarter * 4 + lax.rem(col + far_first(offset), 4)
            post_column(sent_two, got_two, 1, peer_col, column_sems.at[col])
            return inner

        lax.fori_loop(0, 4, send_quarter, 0)
        return carry

    lax.fori_loop(0, 4, quarter_out, 0)

    def linear(group, carry):
        place = pl.ds(pl.multiple_of(group * 8, 8), 8)
        shape = (8, BLOCK_Y)
        wave_x = col * BLOCK_X + group * 8 + lax.broadcasted_iota(jnp.int32, shape, 0)
        index_y = row * BLOCK_Y + lax.broadcasted_iota(jnp.int32, shape, 1)
        signed_y = jnp.where(index_y < LENGTH // 2, index_y, index_y - LENGTH)
        damping, weight_a, weight_b, weight_c = section_weights(wave_x, signed_y)
        weight_last[place, :] = weight_c
        for part in range(2):
            target[part, place, :] = (
                damping * start_field[part, place, :]
                + weight_a * start_term[part, place, :]
                + 2.0 * weight_b * (first_term[part, place, :] + second_term[part, place, :])
            )
        return carry

    lax.fori_loop(0, BLOCK_X // 8, linear, 0)
    turn_tables(1)

    lane = lax.broadcasted_iota(jnp.int32, (8, 128), 1)
    upper = lane >= 64

    def columns_in(step_in, carry):
        group = col_at(step_in, -1)
        await_bytes(
            got_two.at[pl.ds(group * ROWS * LINES, ROWS * LINES)], column_sems.at[group]
        )
        spread = []
        for high_bit in range(2):
            start = (high_bit * 8 + group * 16) * LINES
            spread.append(
                spread_lines(
                    [got_two[pl.ds(start + l, 8, stride=LINES), :] for l in range(LINES)],
                    upper,
                )
            )
        column = [None] * 64
        for step in range(32):
            other = spread[1][step]
            moved = total(
                [
                    scaled(cosine_of(step, 64), other),
                    scaled(sine_of(step, 64), turned(other, upper)) if step else None,
                ]
            )
            column[step] = spread[0][step] + moved
            column[step + 32] = spread[0][step] - moved
        place = pl.multiple_of(group * 8, 8)
        for step in range(PAIRS):
            value = column[step]
            if step % 32 == 0:
                real_part = jnp.where(upper, 0.0, value)
                imag_part = jnp.where(upper, 0.0, pltpu.roll(value, 64, 1))
            else:
                mirror = column[64 - step]
                real_part = jnp.where(upper, pltpu.roll(mirror, 64, 1), value)
                imag_part = jnp.where(upper, -mirror, pltpu.roll(value, 64, 1))
            points[step, pl.ds(place, 8), :] = real_part
            points[step, pl.ds(place + 128, 8), :] = imag_part
        return carry

    lax.fori_loop(0, 16, columns_in, 0)

    first_field = lax.broadcasted_iota(jnp.int32, (128, 128), 1) % 64 < 32

    def column_products(step, carry):
        for index in [11 * step + k for k in range(11)]:
            high, low = split(points[index])
            wide = jnp.dot(
                table[index],
                jnp.concatenate([high, low], axis=1),
                preferred_element_type=FULL,
            )
            grid = (wide[:128, 128:] + wide[128:, :128]) + wide[:128, :128]
            from_left = pltpu.roll(grid, 32, 1)
            from_right = pltpu.roll(grid, 96, 1)
            product = jnp.where(
                first_field, grid * from_right, (grid - from_left) * (grid + from_left)
            )
            both = jnp.concatenate(split(product), axis=1)
            wide = jnp.dot(
                back[index],
                jnp.concatenate([both, both], axis=0),
                preferred_element_type=FULL,
            )
            points[index] = wide[:, 128:] + wide[:, :128]
        return carry

    lax.fori_loop(0, PAIRS // 11, column_products, 0)

    def columns_out(step_out, carry):
        group = col_at(step_out, 1)
        place = pl.multiple_of(group * 8, 8)
        column = [None] * 64
        for step in range(PAIRS):
            real_part = points[step, pl.ds(place, 8), :]
            imag_part = points[step, pl.ds(place + 128, 8), :]
            column[step] = jnp.where(upper, pltpu.roll(imag_part, 64, 1), real_part)
            if step % 32:
                column[64 - step] = jnp.where(
                    upper, -imag_part, pltpu.roll(real_part, 64, 1)
                )
        sums, gaps = [], []
        for step in range(32):
            sums.append(column[step] + column[step + 32])
            gap = column[step] - column[step + 32]
            gaps.append(
                total(
                    [
                        scaled(cosine_of(step, 64), gap),
                        scaled(-sine_of(step, 64), turned(gap, upper)) if step else None,
                    ]
                )
            )
        for high_bit, values in enumerate((sums, gaps)):
            start = (high_bit * 8 + group * 16) * LINES
            for l, value in enumerate(gather_lines(values, upper)):
                sent_three[pl.ds(start + l, 8, stride=LINES), :] = value
        post_column(sent_three, got_three, 2, group, recv_sems.at[0])
        return carry

    lax.fori_loop(0, 16, columns_out, 0)

    await_bytes(got_three, recv_sems.at[0])

    def collect(l, carry):
        for quarter in range(4):
            for group in range(4):
                start = (quarter * 64 + group * 16) * LINES + l
                top, rest = split(
                    jnp.concatenate(
                        [
                            got_three[pl.ds(start, 8, stride=LINES), :],
                            got_three[pl.ds(start + 8 * LINES, 8, stride=LINES), :],
                        ]
                    )
                )
                place = pl.ds(pl.multiple_of(l * 64, 64) + group * 16, 16)
                lanes = slice(quarter * 128, quarter * 128 + 128)
                lines_high[place, lanes] = top
                lines_low[place, lanes] = rest
        return carry

    lax.fori_loop(0, LINES, collect, 0)

    for part, full in enumerate((lines_full, lines_imag)):
        wide = slice(256 * part, 256 * part + 256)
        full[...] = times(
            lines_high[...], lines_low[...], third_table[0, :, wide], third_table[1, :, wide]
        )

    def line_out(l):
        place = pl.ds(pl.multiple_of(l * 64, 64), 64)
        real, imag = lines_full[place, :], lines_imag[place, :]
        out_real = real * turn_cos + imag * turn_sin
        out_imag = imag * turn_cos - real * turn_sin
        high, low = split(jnp.concatenate([out_real, out_imag], axis=0))
        value = times(last_table[0], last_table[1], high, low)
        full_x = jnp.full((1, 128), l * BLOCK_X + own_line, jnp.int32)
        kappa_x = wave_scale * full_x.astype(FULL) / LENGTH
        scale = jnp.where(keep_y & (3 * full_x < LENGTH), 1.0 / LENGTH, 0.0)
        weight_cross = (kappa_x * kappa_x - kappa_y * kappa_y) * scale
        weight_gap = kappa_x * kappa_y * scale
        sent_four[l] = weight_cross * value[:, :128] + weight_gap * value[:, 128:]

        def send_term(step, inner):
            block = lax.rem(kept_row + step, KEPT)
            post(
                sent_four.at[l, pl.ds(pl.multiple_of(block * 8, 8), 8)],
                got_four.at[pl.ds(pl.multiple_of(own_line * 8, 8), 8)],
                3,
                jnp.where(block < KEPT // 2, block, block + (ROWS - KEPT)),
                l,
                recv_sems.at[1],
            )
            return inner

        lax.fori_loop(0, KEPT, send_term, 0)

    def line_out_step(step, carry):
        l = col_at(step, 1)

        @pl.when(l < LINES)
        def _():
            line_out(l)

        return carry

    lax.fori_loop(0, COLS, line_out_step, 0)

    @pl.when(holds)
    def _():
        await_bytes(got_four, recv_sems.at[1])

        def finish(group, carry):
            place = pl.ds(pl.multiple_of(group * 8, 8), 8)
            for part in range(2):
                for quarter in range(4):
                    lanes = slice(quarter * 128, quarter * 128 + 128)
                    start = pl.multiple_of(group * 64, 64) + (part * 4 + quarter)
                    target[part, place, lanes] = (
                        target[part, place, lanes]
                        + weight_last[place, lanes] * got_four[pl.ds(start, 8, stride=8), :]
                    )
            return carry

        lax.fori_loop(0, BLOCK_X // 8, finish, 0)
        others = sent_one.at[pl.ds(0, (DEVICES - 1) * 8)]
        await_bytes(others, send_sems.at[0])
        await_bytes(sent_four.at[0, pl.ds(0, KEPT * 8 - 8)], send_sems.at[3])
        await_bytes(sent_four.at[pl.ds(0, LINES - 1)], send_sems.at[3])

    @pl.when(jnp.logical_not(holds))
    def _():
        await_bytes(sent_four, send_sems.at[3])

    for phase, sent in ((1, sent_two), (2, sent_three)):
        await_bytes(sent.at[pl.ds(0, (DEVICES - 1) * LINES)], send_sems.at[phase])


def per_device(start_field, section_field, start_term, first_term, second_term):
    shape = (2, BLOCK_X, BLOCK_Y)
    fields = [
        field.reshape(shape)
        for field in (start_field, section_field, start_term, first_term, second_term)
    ]
    constants = [jnp.asarray(table) for table in tables()]
    vmem = pl.BlockSpec(memory_space=pltpu.VMEM)
    result = pl.pallas_call(
        section_kernel,
        out_shape=jax.ShapeDtypeStruct(shape, FULL),
        in_specs=[vmem] * (len(fields) + len(constants)),
        out_specs=vmem,
        scratch_shapes=[
            pltpu.VMEM((BLOCK_X * 8, 128), FULL),
            pltpu.VMEM((LINES, KEPT * 8, 128), FULL),
            pltpu.VMEM((DEVICES * LINES, 128), FULL),
            pltpu.VMEM((DEVICES * LINES, 128), FULL),
            pltpu.VMEM((DEVICES * LINES, 128), FULL),
            pltpu.VMEM((DEVICES * LINES, 128), FULL),
            pltpu.VMEM((LINES, KEPT * 8, 128), FULL),
            pltpu.VMEM((BLOCK_X * 8, 128), FULL),
            pltpu.VMEM((LINES * 64, 512), HIGH),
            pltpu.VMEM((LINES * 64, 512), HIGH),
            pltpu.VMEM((LINES * 64, 256), FULL),
            pltpu.VMEM((LINES * 64, 256), FULL),
            pltpu.VMEM((PAIRS, 256, 128), FULL),
            pltpu.VMEM((PAIRS, 256, 256), HIGH),
            pltpu.VMEM((PAIRS, 256, 256), HIGH),
            pltpu.VMEM((BLOCK_X, BLOCK_Y), FULL),
            pltpu.SemaphoreType.DMA((4,)),
            pltpu.SemaphoreType.DMA((2,)),
            pltpu.SemaphoreType.DMA((LINES,)),
            pltpu.SemaphoreType.DMA((COLS,)),
        ],
        compiler_params=pltpu.CompilerParams(
            has_side_effects=True, vmem_limit_bytes=56 * 2**20
        ),
        name="section",
    )(*fields, *constants)
    return result.reshape((1,) + shape)


def solution(mesh):
    spec = P(None, None, "col", "row")
    return jax.shard_map(
        per_device,
        mesh=mesh,
        in_specs=(spec,) * 5,
        out_specs=spec,
        check_vma=False,
    )
```
